128 devices in a mesh: lat: 8 (over y, x_hi), lon: 16 (over x_lo, z, core).
Axes of the slice: x: 4 (x_hi: 2, x_lo: 2; x = x_hi * 2 + x_lo), y: 4, z: 4, core: 2. Of those that a mesh axis runs over, the one named last changes fastest.
Arguments:
- adjoint_in: float32 [4, 79, 64, 2048], P(None, None, 'lat', 'lon'), may hold values from -6 to 6
- fractions: bfloat16 [4, 4, 79, 64, 2048], P(None, None, None, 'lat', 'lon'), may hold values from 0 to 0.95, as said below
- profiles: bfloat16 [2, 79, 64, 2048], P(None, None, 'lat', 'lon'), may hold values from 0.099609375 to 1
- kernel: bfloat16 [79, 79], replicated, may hold values from -0.625 to 0.625
- obs_weights: bfloat16 [79, 524288], P(None, ('lat', 'lon')), may hold values from 0.099609375 to 1.5
- obs_resid: bfloat16 [4, 524288], P(None, ('lat', 'lon')), may hold values from -5 to 5
- obs_cols: int32 [524288], P(('lat', 'lon')), may hold values from 0 to 1023
- obs_owner: int32 [65536, 1], P(('lat', 'lon')), may hold values from 0 to 127; in each aligned block of 512 rows (0 to 511, 512 to 1023, ...) at most 6 rows name the same one
- obs_count: int32 [65536], P(('lat', 'lon')), may hold values from 5 to 8
- lat_matrix: bfloat16 [64, 64], replicated, as said below
- lon_matrix: bfloat16 [2048, 2048], P('lon'), as said below
Outputs:
- adjoint_out: float32 [4, 79, 64, 2048], P(None, None, 'lat', 'lon')
- smoothed_gradient: float32 [4, 64, 2048], P(None, 'lat', 'lon')
The draws below stay inside these ranges and needn't reach their ends.
Inputs may be any that keep to these rules, and one draw needn't show every extreme that they name: `fractions`: fractions are nonnegative and the four of one cell and step sum to at most 0.95. `obs_owner`: owners are numbered as lat index times 16 plus lon index. Among the blocks of one device at most 6 share an owner. `obs_cols`: A tile's columns are numbered row by row: row within the tile times 128 plus column within the tile. The first obs_count slots of a block are valid, the others are padding. `lat_matrix`: Symmetric. `lon_matrix`: Symmetric.
All inputs are finite; a program needn't handle non-finite values.
Results may differ from the reference program's by a relative error of at most 0.0041.
Values may be sent and summed in bfloat16 or wider, within the bound.
A program may use at most 192 MiB of HBM per device.

```python
import math
import jax
import jax.numpy as jnp
import numpy as np
from jax import lax

TRACERS = 4
LEV = 79
STEPS = 4
SLOTS = 8
CAPACITY = 6
LAT_DEV = 8
LON_DEV = 128
BLK_DEV = 512
NLAT = 64
NLON = 2048
CELLS_DEV = 1024
NBLK = 65536
NSND = 524288
N_LON = 16
DEVICES = 128


def symmetric_matrix(key, matrix_order):
    key_one, key_two = jax.random.split(key)
    noise_part = jax.random.normal(key_one, (matrix_order, matrix_order), jnp.float32)
    diagonal = jax.random.uniform(key_two, (matrix_order,), jnp.float32, 1.0, 2.0)
    scaled = (noise_part + noise_part.T) * (0.3 / math.sqrt(matrix_order))
    return (jnp.diag(diagonal) + scaled).astype(jnp.bfloat16)


def draw_fractions(key, part):
    key_one, key_two = jax.random.split(jax.random.fold_in(key, 5))
    shares = jax.random.uniform(key_one, (STEPS, 4, LEV, NLAT, NLON), jnp.float32, 0.05, 1.0)
    totals = jax.random.uniform(key_two, (STEPS, 1, LEV, NLAT, NLON), jnp.float32, 0.3, 0.95)
    return (totals * shares / jnp.sum(shares, axis=1, keepdims=True)).astype(jnp.bfloat16)


def draw_lat_matrix(key, part):
    return symmetric_matrix(jax.random.fold_in(key, 11), NLAT)


def draw_lon_matrix(key, part):
    return symmetric_matrix(jax.random.fold_in(key, 23), NLON)


def plant(entries, rng, low, largest):
    longest = entries.shape.index(max(entries.shape))
    spots = []
    for shift in (0, 1):
        where = [jax.random.randint(jax.random.fold_in(rng, axis), (), 0, length) for axis, length in enumerate(entries.shape)]
        where[longest] = (where[longest] + shift) % entries.shape[longest]
        spots.append(tuple(where))
    return entries.at[spots[0]].set(low).at[spots[1]].set(largest)


def block_levels(own_key, dims, cuts, low, top_value):
    loudness, own = 1.0, jax.random.fold_in(own_key, 6)
    for position, shards_of in cuts:
        heights = jnp.exp(jax.random.uniform(jax.random.fold_in(own, position), (shards_of,), jnp.float32, low / len(cuts), top_value / len(cuts)))
        loudness = loudness * jnp.repeat(heights, dims[position] // shards_of).reshape([-1 if axis == position else 1 for axis in range(len(dims))])
    return loudness


def routed_block(rng, own, number, rows, count, top, reach, slope):
    ranking = jax.random.permutation(rng, count)
    heavy_load, common = load_shares(count, rows * top, reach, slope, True), load_shares(count, rows * top, reach, slope, False)
    places = jnp.arange(count)

    def named(lengths, turn):
        used = int((lengths > 0).sum())
        fixed = max(1, used // 4)
        passed = fixed + (places - fixed + turn * (used - fixed)) % max(1, count - fixed)
        return jnp.zeros((count,), jnp.int32).at[ranking[jnp.where(places < fixed, places, passed)]].set(jnp.asarray(lengths, jnp.int32))

    lengths = jnp.where(number % 4 == 0, named(heavy_load, number // 4), named(common, number - number // 4 - 1))
    mixed = jax.random.permutation(jax.random.fold_in(own, 3), count)
    donor, taker = mixed[0:count // 2 * 2:2], mixed[1:count // 2 * 2:2]
    margin = jnp.minimum(lengths[donor] - 1, reach - lengths[taker]) // 2
    margin = jnp.where((donor == ranking[0]) | (taker == ranking[0]) | (lengths[taker] == 0), 0, jnp.maximum(margin, 0))
    passed = jax.random.randint(jax.random.fold_in(own, 4), (count // 2,), 0, 1 << 20) % (margin + 1)
    lengths = lengths.at[donor].add(-passed).at[taker].add(passed)
    items = jnp.searchsorted(jnp.cumsum(lengths), jnp.arange(rows * top), side="right").astype(jnp.int32)
    grid = items.reshape(top, rows).T
    grid = grid[jax.random.permutation(jax.random.fold_in(own, 1), rows)]
    turn = jax.random.randint(jax.random.fold_in(own, 2), (rows, 1), 0, top)
    return jnp.take_along_axis(grid, (jnp.arange(top)[None, :] + turn) % top, axis=1)


def load_shares(count, total, reach, skew, full):
    loads = [(1 << 20) // math.isqrt(rank ** skew) + 1 for rank in range(1, count + 1)]
    largest = reach if full else min(reach, max(-(-total // count), total * loads[0] // sum(loads)))
    least = 1 if total - largest >= count - 1 else 0
    holding, surplus = [largest] + [least] * (count - 1), total - largest - least * (count - 1)
    while surplus > 0:
        movable = [i for i in range(1, count) if holding[i] < largest] or [i for i in range(1, count) if holding[i] < reach]
        whole, remaining = sum([loads[i] for i in movable]), surplus
        for i in movable:
            extra = min(reach - holding[i], max(1, remaining * loads[i] // whole), surplus)
            holding[i] = holding[i] + extra
            surplus = surplus - extra
    return np.array(holding)


def centred(rng, extent, width, most, cuts=(), dtype=jnp.bfloat16):
    factor_of = block_levels(rng, extent, cuts, -0.22, 0.18) if cuts else 1.0
    values = jax.random.normal(rng, extent, jnp.float32) * width * factor_of
    return jnp.minimum(jnp.maximum(values, -most), most).astype(dtype)


def setup_inputs(seed: int = 0) -> dict:
    seeds = jax.random.split(jax.random.key(seed), 12)
    adjoint_in = centred(seeds[0], (TRACERS, LEV, NLAT, NLON), 1.0, 6.0, ((2, 8), (3, 16)), jnp.float32)
    fractions = draw_fractions(jax.random.fold_in(seeds[11], 71), 0)
    profiles = jnp.clip(jnp.exp(math.log(1.0) - 2.306499 * jax.random.uniform(seeds[2], (2, LEV, NLAT, NLON), jnp.float32) ** block_levels(seeds[2], (2, LEV, NLAT, NLON), ((2, 8), (3, 16)), -0.2, 0.2)), 0.099609375, 1.0).astype(jnp.bfloat16)
    kernel = centred(seeds[3], (LEV, LEV), LEV ** -0.5, 0.625)
    obs_weights = jnp.clip(0.099609375 + 1.4003906 * jax.random.uniform(seeds[4], (LEV, NSND), jnp.float32) ** block_levels(seeds[4], (LEV, NSND), ((1, 128),), -0.2, 0.2), 0.099609375, 1.5).astype(jnp.bfloat16)
    obs_resid = centred(seeds[5], (TRACERS, NSND), 1.0, 5.0, ((1, 128),))
    obs_cols = plant(jax.random.randint(seeds[6], (NSND,), 0, CELLS_DEV), jax.random.fold_in(seeds[6], 1), 0, CELLS_DEV - 1).astype(jnp.int32)
    obs_owner_keys = jax.random.split(jax.random.fold_in(seeds[7], 1), NBLK // BLK_DEV)
    obs_owner_turns = jax.random.permutation(jax.random.fold_in(seeds[7], 3), NBLK // BLK_DEV)
    obs_owner = jax.vmap(lambda own, number: routed_block(jax.random.fold_in(seeds[7], 2), own, number, BLK_DEV, DEVICES, 1, CAPACITY, 2))(obs_owner_keys, obs_owner_turns).reshape((NBLK, 1))
    obs_count = plant(jax.random.randint(seeds[8], (NBLK,), 5, SLOTS + 1), jax.random.fold_in(seeds[8], 1), 5, SLOTS).astype(jnp.int32)
    lat_matrix = draw_lat_matrix(jax.random.fold_in(seeds[11], 71), 0)
    lon_matrix = draw_lon_matrix(jax.random.fold_in(seeds[11], 71), 0)
    return dict(adjoint_in=adjoint_in, fractions=fractions, profiles=profiles, kernel=kernel, obs_weights=obs_weights, obs_resid=obs_resid, obs_cols=obs_cols, obs_owner=obs_owner, obs_count=obs_count, lat_matrix=lat_matrix, lon_matrix=lon_matrix)


def convect(adjoint, kernel, entrain, detrain):
    lowered = (detrain * adjoint).astype(jnp.bfloat16)
    mixing = jnp.einsum("kj,tkyx->tjyx", kernel.astype(jnp.float32), lowered.astype(jnp.float32), precision=lax.Precision.HIGHEST)
    return adjoint + entrain * mixing


def transport(field_in, fraction):
    east_side = jnp.roll(field_in, -1, axis=3)
    west_side = jnp.roll(field_in, 1, axis=3)
    padded = jnp.pad(field_in, ((0, 0), (0, 0), (1, 1), (0, 0)))
    north_side = padded[:, :, 2:, :]
    south_side = padded[:, :, :-2, :]
    remain = 1.0 - fraction[0] - fraction[1] - fraction[2] - fraction[3]
    return (remain * field_in + fraction[0] * east_side + fraction[1] * west_side
            + fraction[2] * north_side + fraction[3] * south_side)


def sounding_forcing(obs_weights, obs_resid, obs_cols, obs_owner, obs_count):
    blocks = obs_count.shape[0]
    slot_index = jnp.tile(jnp.arange(SLOTS).astype(jnp.int32), blocks)
    owner_device = jnp.repeat(obs_owner[:, 0], SLOTS).astype(jnp.int32)
    live_count = jnp.repeat(obs_count, SLOTS).astype(jnp.int32)
    row_index = (owner_device // N_LON) * LAT_DEV + obs_cols // LON_DEV
    col_index = (owner_device % N_LON) * LON_DEV + obs_cols % LON_DEV
    cell_index = jnp.where(slot_index < live_count, row_index * NLON + col_index, NLAT * NLON).astype(jnp.int32)
    contrib = obs_weights.astype(jnp.float32)[None, :, :] * obs_resid.astype(jnp.float32)[:, None, :]
    flattened = jnp.zeros((TRACERS, LEV, NLAT * NLON), jnp.float32)
    flattened = flattened.at[:, :, cell_index].add(contrib, mode="drop")
    return flattened.reshape(TRACERS, LEV, NLAT, NLON)


def reference(adjoint_in, fractions, profiles, kernel, obs_weights, obs_resid, obs_cols, obs_owner, obs_count, lat_matrix, lon_matrix):
    entrain = profiles[0].astype(jnp.float32)
    detrain = profiles[1].astype(jnp.float32)
    forcing = sounding_forcing(obs_weights, obs_resid, obs_cols, obs_owner, obs_count)
    adjoint = adjoint_in
    surface = jnp.zeros((TRACERS, NLAT, NLON), jnp.float32)
    for step_index in range(STEPS - 1, -1, -1):
        fraction = fractions[step_index].astype(jnp.float32)
        adjoint = transport(convect(adjoint, kernel, entrain, detrain), fraction)
        if step_index == 0:
            adjoint = adjoint + forcing
        surface = surface + adjoint[:, 0]
    surface_low = surface.astype(jnp.bfloat16)
    lon_smoothed = jnp.einsum("tyx,xj->tyj", surface_low.astype(jnp.float32), lon_matrix.astype(jnp.float32), precision=lax.Precision.HIGHEST).astype(jnp.bfloat16)
    smoothed_gradient = jnp.einsum("iy,tyj->tij", lat_matrix.astype(jnp.float32), lon_smoothed.astype(jnp.float32), precision=lax.Precision.HIGHEST)
    return adjoint, smoothed_gradient
```

```python
import functools

import jax
import jax.numpy as jnp
from jax import lax
from jax.experimental import pallas as pl
from jax.experimental.pallas import tpu as pltpu
from jax.sharding import PartitionSpec as P

STEPS = 4
CAPACITY = 6
SLOTS = 8
MESH = pl.DeviceIdType.MESH
F32 = jnp.float32
BF16 = jnp.bfloat16
VMEM = pl.BlockSpec(memory_space=pltpu.VMEM)
SMEM = pl.BlockSpec(memory_space=pltpu.SMEM)


def padded(levels):
    return -(-levels // 16) * 16


def pack_kernel(levels, tracers, devices, w_ref, r_ref, c_ref, owner_ref, count_ref, out_ref, feat, rows, seen):
    blocks = owner_ref.shape[0]
    lanes = 128
    per_chunk = lanes // SLOTS
    feat[0:levels, :] = w_ref[...].astype(F32)
    feat[levels : levels + tracers, :] = r_ref[...].astype(F32)
    cell = c_ref[...]
    feat[levels + tracers : levels + tracers + 1, :] = (cell // lanes).astype(F32)
    feat[levels + tracers + 1 : levels + tracers + 2, :] = (cell % lanes).astype(F32)
    rows[...] = jnp.zeros_like(rows)

    @pl.loop(0, devices)
    def _(d):
        seen[d] = 0

    slot = lax.broadcasted_iota(jnp.int32, (SLOTS, lanes), 0)

    @pl.loop(0, blocks // per_chunk)
    def _(chunk):
        at = pl.multiple_of(chunk * lanes, lanes)
        turned = feat[:, pl.ds(at, lanes)].T
        for i in range(per_chunk):
            b = chunk * per_chunk + i
            owner = owner_ref[b]
            rank = seen[owner]
            seen[owner] = rank + 1
            place = pl.multiple_of((owner * CAPACITY + rank) * SLOTS, SLOTS)
            block = turned[i * SLOTS : (i + 1) * SLOTS, :]
            rows[pl.ds(place, SLOTS), :] = jnp.where(slot < count_ref[b], block, 0.0)

    width = levels + tracers + 2
    spare = lanes - width
    lane = lax.broadcasted_iota(jnp.int32, (SLOTS, lanes), 1)

    @pl.loop(0, devices, unroll=4)
    def _(d):
        base = d * (CAPACITY * SLOTS)
        got = [rows[pl.ds(pl.multiple_of(base + i * SLOTS, SLOTS), SLOTS), :] for i in range(CAPACITY)]
        pieces = []
        for i in range(4):
            extra = got[4 + i // 2]
            shift = width if i % 2 == 0 else width - spare
            pieces.append(jnp.where(lane < width, got[i], pltpu.roll(extra, shift, 1)))
        out_ref[d] = jnp.concatenate(pieces, axis=0).astype(BF16)


def steps_kernel(
    tracers, levels, lat_rows,
    adj_ref, frac_ref, prof_ref, ker_ref,
    state, surf_ref,
    mixed, fracs, profs, square,
    lat_send, lat_recv, lon_send, lon_recv,
    lat_ss, lat_rs, lon_ss, lon_rs,
):
    lanes = 128
    lev = padded(levels)
    rows = levels * lat_rows
    lat, lon = lax.axis_index("lat"), lax.axis_index("lon")
    nlat, nlon = lax.axis_size("lat"), lax.axis_size("lon")
    up, down = lax.rem(lat + 1, nlat), lax.rem(lat + nlat - 1, nlat)
    east, west = lax.rem(lon + 1, nlon), lax.rem(lon + nlon - 1, nlon)
    barrier = pltpu.get_barrier_semaphore()
    pl.semaphore_signal(barrier, inc=1, device_id={"lat": up}, device_id_type=MESH)
    pl.semaphore_signal(barrier, inc=1, device_id={"lat": down}, device_id_type=MESH)
    pl.semaphore_signal(barrier, inc=1, device_id={"lon": east}, device_id_type=MESH)
    pl.semaphore_signal(barrier, inc=1, device_id={"lon": west}, device_id_type=MESH)

    @pl.when(lat == 0)
    def _():
        for n in range(STEPS):
            lat_recv[n, 0] = jnp.zeros((lev, tracers * lanes), BF16)

    @pl.when(lat == nlat - 1)
    def _():
        for n in range(STEPS):
            lat_recv[n, 1] = jnp.zeros((lev, tracers * lanes), BF16)

    square[...] = jnp.zeros_like(square)
    square[0:levels, 0:levels] = ker_ref[...].astype(F32)
    turned = square[...].T[0:lev, 0:lev].astype(BF16)
    pad = lev * lat_rows - rows
    for i in range(2):
        profs[i, 0:rows, :] = prof_ref[i * rows : (i + 1) * rows, :].astype(F32)
        profs[i, rows : rows + pad, :] = jnp.zeros((pad, lanes), F32)
    for f in range(4):
        fracs[f, rows : rows + pad, :] = jnp.zeros((pad, lanes), F32)
    for y in range(lat_rows):
        state[y, levels:lev, :] = jnp.zeros((lev - levels, tracers * lanes), F32)
        for t in range(tracers):
            state[y, 0:levels, t * lanes : (t + 1) * lanes] = adj_ref[pl.ds(t * rows + y, levels, stride=lat_rows), :]
    surf_ref[...] = jnp.zeros_like(surf_ref)
    pl.semaphore_wait(barrier, 4)

    lane = lax.broadcasted_iota(jnp.int32, (lev, lanes), 1)
    half = lev // 2
    lane_half = lax.broadcasted_iota(jnp.int32, (half, lanes), 1)

    def lat_copy(i, side):
        return pltpu.make_async_remote_copy(
            src_ref=lat_send.at[i, side],
            dst_ref=lat_recv.at[i, 1 - side],
            send_sem=lat_ss.at[i, side],
            recv_sem=lat_rs.at[i, 1 - side],
            device_id={"lat": up if side else down},
            device_id_type=MESH,
        )

    def lon_copy(i, side):
        return pltpu.make_async_remote_copy(
            src_ref=lon_send.at[i, side],
            dst_ref=lon_recv.at[i, 1 - side],
            send_sem=lon_ss.at[i, side],
            recv_sem=lon_rs.at[i, 1 - side],
            device_id={"lon": east if side else west},
            device_id_type=MESH,
        )

    def step(i, _):
        n = STEPS - 1 - i
        columns = [jnp.zeros((lev, lanes), F32), jnp.zeros((lev, lanes), F32)]
        order = [0, lat_rows - 1] + list(range(1, lat_rows - 1))
        for y in order:
            entrain = profs[0, pl.ds(y, lev, stride=lat_rows), :]
            detrain = profs[1, pl.ds(y, lev, stride=lat_rows), :]
            lowered = (jnp.concatenate([detrain] * tracers, axis=1) * state[y]).astype(BF16)
            mixing = jnp.dot(turned, lowered, preferred_element_type=F32)
            mixed[y] = state[y] + jnp.concatenate([entrain] * tracers, axis=1) * mixing
            if y == 0:
                lat_send[i, 0] = mixed[y].astype(BF16)

                @pl.when(lat > 0)
                def _():
                    lat_copy(i, 0).start()

            if y == lat_rows - 1:
                lat_send[i, 1] = mixed[y].astype(BF16)

                @pl.when(lat < nlat - 1)
                def _():
                    lat_copy(i, 1).start()

        for y in range(lat_rows):
            for t in range(tracers):
                at = y * tracers + t
                tile = mixed[y, :, t * lanes : (t + 1) * lanes]
                west_edge = tile if at == 0 else pltpu.roll(tile, at, 1)
                columns[0] = jnp.where(lane == at, west_edge, columns[0])
                columns[1] = jnp.where(lane == at, pltpu.roll(tile, at + 1, 1), columns[1])
        for side in range(2):
            lon_send[i, side] = columns[side]
            lon_copy(i, side).start()
        for f in range(4):
            at = pl.multiple_of((n * 4 + f) * rows, 8)
            fracs[f, 0:rows, :] = frac_ref[pl.ds(at, rows), :].astype(F32)
        lon_copy(i, 0).wait_recv()
        lon_copy(i, 1).wait_recv()

        def advance(y):
            for h in range(2):
                ks = slice(h * half, (h + 1) * half)
                f = [fracs[j, pl.ds(h * half * lat_rows + y, half, stride=lat_rows), :] for j in range(4)]
                remain = 1.0 - f[0] - f[1] - f[2] - f[3]
                from_west, from_east = lon_recv[i, 0, ks, :], lon_recv[i, 1, ks, :]
                for t in range(tracers):
                    ts = slice(t * lanes, (t + 1) * lanes)
                    at = y * tracers + t
                    here = mixed[y, ks, ts]
                    side_e = jnp.where(
                        lane_half == lanes - 1,
                        jnp.broadcast_to(from_east[:, at : at + 1], (half, lanes)),
                        pltpu.roll(here, lanes - 1, 1),
                    )
                    side_w = jnp.where(
                        lane_half == 0,
                        jnp.broadcast_to(from_west[:, at : at + 1], (half, lanes)),
                        pltpu.roll(here, 1, 1),
                    )
                    north = lat_recv[i, 1, ks, ts].astype(F32) if y == lat_rows - 1 else mixed[y + 1, ks, ts]
                    south = lat_recv[i, 0, ks, ts].astype(F32) if y == 0 else mixed[y - 1, ks, ts]
                    state[y, ks, ts] = remain * here + f[0] * side_e + f[1] * side_w + f[2] * north + f[3] * south

        for y in range(1, lat_rows - 1):
            advance(y)

        @pl.when(lat < nlat - 1)
        def _():
            lat_copy(i, 0).wait_recv()

        @pl.when(lat > 0)
        def _():
            lat_copy(i, 1).wait_recv()

        advance(0)
        advance(lat_rows - 1)

        @pl.when(i < STEPS - 1)
        def _():
            for y in range(lat_rows):
                surf_ref[y] += state[y, 0:8, :]

        return 0

    lax.fori_loop(0, STEPS, step, 0)
    for i in range(STEPS):
        for side in range(2):
            lon_copy(i, side).wait_send()

        @pl.when(lat > 0)
        def _():
            lat_copy(i, 0).wait_send()

        @pl.when(lat < nlat - 1)
        def _():
            lat_copy(i, 1).wait_send()


def forcing_kernel(tracers, levels, lat_rows, group, recv_ref, state_ref, surf_ref, out_ref, low_ref, acc, rows, lhs, rhs, flat):
    lanes = 128
    lev = padded(levels)
    devices = recv_ref.shape[0]
    width = levels + tracers + 2
    spare = lanes - width
    slots = CAPACITY * SLOTS
    acc[...] = state_ref[...].reshape(acc.shape)
    lane8 = lax.broadcasted_iota(jnp.int32, (SLOTS, lanes), 1)
    lane16 = lax.broadcasted_iota(jnp.int32, (16, lanes), 1).astype(F32)

    @pl.loop(0, devices // group)
    def _(g):
        for p in range(group):
            block = recv_ref[g * group + p].astype(F32)
            quarter = [block[i * SLOTS : (i + 1) * SLOTS] for i in range(4)]
            for i in range(4):
                rows[p * slots + i * SLOTS : p * slots + (i + 1) * SLOTS, :] = quarter[i]
            for i in range(2):
                low = pltpu.roll(quarter[2 * i], lanes - width, 1)
                high = pltpu.roll(quarter[2 * i + 1], lanes - width + spare, 1)
                at = p * slots + (4 + i) * SLOTS
                rows[at : at + SLOTS, :] = jnp.where(lane8 < spare, low, high)
        for c in range(group * slots // lanes):
            turned = rows[c * lanes : (c + 1) * lanes, :].T
            weights = turned[0:lev, :]
            row = turned[levels + tracers : levels + tracers + 1, :]
            for y in range(lat_rows):
                lhs[y * lev : (y + 1) * lev, c * lanes : (c + 1) * lanes] = jnp.where(row == y, weights, 0.0).astype(BF16)
        for s in range(group * slots // 16):
            here = rows[s * 16 : (s + 1) * 16, :]
            col = jnp.broadcast_to(here[:, width - 1 : width], (16, lanes)) == lane16
            for t in range(tracers):
                value = jnp.broadcast_to(here[:, levels + t : levels + t + 1], (16, lanes))
                rhs[s * 16 : (s + 1) * 16, t * lanes : (t + 1) * lanes] = jnp.where(col, value, 0.0).astype(BF16)
        acc[...] += jnp.dot(lhs[...], rhs[...], preferred_element_type=F32)

    for y in range(lat_rows):
        for t in range(tracers):
            ts = slice(t * lanes, (t + 1) * lanes)
            out_ref[pl.ds(t * levels * lat_rows + y, levels, stride=lat_rows), :] = acc[y * lev : y * lev + levels, ts]
            at = y * tracers + t
            flat[at : at + 1, :] = surf_ref[y, 0:1, ts] + acc[y * lev : y * lev + 1, ts]
    low_ref[...] = flat[...].astype(BF16)


def smooth_kernel(tracers, lat_rows, low_ref, lonm_ref, latm_ref, out_ref, lon_got, lat_got, own, ss_lon, rs_lon, ss_lat, rs_lat):
    lanes = 128
    lat, lon = lax.axis_index("lat"), lax.axis_index("lon")
    nlat, nlon = lax.axis_size("lat"), lax.axis_size("lon")
    rows = tracers * lat_rows
    barrier = pltpu.get_barrier_semaphore()
    for d in range(1, nlon):
        pl.semaphore_signal(barrier, inc=1, device_id={"lon": lax.rem(lon + d, nlon)}, device_id_type=MESH)
    for d in range(1, nlat):
        pl.semaphore_signal(barrier, inc=1, device_id={"lat": lax.rem(lat + d, nlat)}, device_id_type=MESH)
    pl.semaphore_wait(barrier, nlon + nlat - 2)

    def lon_copy(d):
        return pltpu.make_async_remote_copy(
            src_ref=low_ref, dst_ref=lon_got.at[d], send_sem=ss_lon.at[d], recv_sem=rs_lon.at[d],
            device_id={"lon": lax.rem(lon + d, nlon)}, device_id_type=MESH,
        )

    def lat_copy(d):
        return pltpu.make_async_remote_copy(
            src_ref=own, dst_ref=lat_got.at[d], send_sem=ss_lat.at[d], recv_sem=rs_lat.at[d],
            device_id={"lat": lax.rem(lat + d, nlat)}, device_id_type=MESH,
        )

    for d in range(1, nlon):
        lon_copy(d).start()

    nrow = latm_ref.shape[0]
    pick = lax.broadcasted_iota(jnp.int32, (rows, nrow), 1) == lat * lat_rows + lax.broadcasted_iota(
        jnp.int32, (rows, nrow), 0
    ) % lat_rows
    own_rows = jnp.dot(jnp.where(pick, 1.0, 0.0).astype(BF16), latm_ref[...], preferred_element_type=F32).astype(BF16)
    spread = lax.broadcasted_iota(jnp.int32, (nrow, nrow * tracers), 0) == lax.broadcasted_iota(
        jnp.int32, (nrow, nrow * tracers), 1
    ) // tracers
    wide = jnp.dot(own_rows, jnp.where(spread, 1.0, 0.0).astype(BF16), preferred_element_type=F32)
    same = lax.broadcasted_iota(jnp.int32, (rows, nrow * tracers), 0) // lat_rows == lax.broadcasted_iota(
        jnp.int32, (rows, nrow * tracers), 1
    ) % tracers
    wide = jnp.where(same, wide, 0.0)

    contract = (((1,), (1,)), ((), ()))

    def part(d, block):
        source = lax.rem(lon - d + nlon, nlon)
        matrix = lonm_ref[:, pl.ds(pl.multiple_of(source * lanes, lanes), lanes)]
        return lax.dot_general(block, matrix, contract, preferred_element_type=F32)

    total = part(0, low_ref[...])
    for d in range(1, nlon):
        lon_copy(d).wait_recv()
        total += part(d, lon_got[d])
    own[...] = total.astype(BF16)
    for d in range(1, nlat):
        lat_copy(d).start()
    lat_got[0] = own[...]
    blocks = []
    for d in range(nlat):
        if d:
            lat_copy(d).wait_recv()
        blocks.append(lat_got[d])
    gathered = jnp.concatenate(blocks, axis=0)
    turned = pltpu.roll(wide, (nlat - 1 - lat) * rows, 1)
    reordered = jnp.concatenate(
        [turned[:, (nlat - 1 - d) * rows : (nlat - d) * rows] for d in range(nlat)], axis=1
    ).astype(BF16)
    smoothed = jnp.dot(reordered, gathered, preferred_element_type=F32)
    out_ref[...] = smoothed.reshape(out_ref.shape)
    for d in range(1, nlon):
        lon_copy(d).wait_send()
    for d in range(1, nlat):
        lat_copy(d).wait_send()


def shards(
    adjoint_in, fractions, profiles, kernel, obs_weights, obs_resid, obs_cols, obs_owner, obs_count, lat_matrix, lon_matrix
):
    tracers, levels, lat_rows, lanes = adjoint_in.shape
    lev = padded(levels)
    nlat, nlon = lax.axis_size("lat"), lax.axis_size("lon")
    devices = nlat * nlon
    blocks = obs_count.shape[0]
    nslots = blocks * SLOTS
    big = dict(vmem_limit_bytes=60 << 20)

    packed = pl.pallas_call(
        functools.partial(pack_kernel, levels, tracers, devices),
        out_shape=jax.ShapeDtypeStruct((devices, 4 * SLOTS, lanes), BF16),
        in_specs=[VMEM, VMEM, VMEM, SMEM, SMEM],
        out_specs=VMEM,
        scratch_shapes=[
            pltpu.VMEM((lanes, nslots), F32),
            pltpu.VMEM((devices * CAPACITY * SLOTS, lanes), F32),
            pltpu.SMEM((devices,), jnp.int32),
        ],
        compiler_params=pltpu.CompilerParams(**big),
        name="pack",
    )(obs_weights, obs_resid, obs_cols.reshape(1, nslots), obs_owner.reshape(blocks), obs_count)
    received = lax.all_to_all(packed, ("lat", "lon"), 0, 0, tiled=True)

    rows = levels * lat_rows
    state, surface = pl.pallas_call(
        functools.partial(steps_kernel, tracers, levels, lat_rows),
        out_shape=(
            jax.ShapeDtypeStruct((lat_rows, lev, tracers * lanes), F32),
            jax.ShapeDtypeStruct((lat_rows, 8, tracers * lanes), F32),
        ),
        in_specs=[VMEM] * 4,
        out_specs=(VMEM, VMEM),
        scratch_shapes=[
            pltpu.VMEM((lat_rows, lev, tracers * lanes), F32),
            pltpu.VMEM((4, lev * lat_rows, lanes), F32),
            pltpu.VMEM((2, lev * lat_rows, lanes), F32),
            pltpu.VMEM((lanes, lanes), F32),
            pltpu.VMEM((STEPS, 2, lev, tracers * lanes), BF16),
            pltpu.VMEM((STEPS, 2, lev, tracers * lanes), BF16),
            pltpu.VMEM((STEPS, 2, lev, lanes), F32),
            pltpu.VMEM((STEPS, 2, lev, lanes), F32),
            pltpu.SemaphoreType.DMA((STEPS, 2)),
            pltpu.SemaphoreType.DMA((STEPS, 2)),
            pltpu.SemaphoreType.DMA((STEPS, 2)),
            pltpu.SemaphoreType.DMA((STEPS, 2)),
        ],
        compiler_params=pltpu.CompilerParams(collective_id=0, has_side_effects=True, **big),
        name="steps",
    )(
        adjoint_in.reshape(tracers * rows, lanes),
        fractions.reshape(STEPS * 4 * rows, lanes),
        profiles.reshape(2 * rows, lanes),
        kernel,
    )

    group = min(16, devices)
    adjoint, low = pl.pallas_call(
        functools.partial(forcing_kernel, tracers, levels, lat_rows, group),
        out_shape=(
            jax.ShapeDtypeStruct((tracers * rows, lanes), F32),
            jax.ShapeDtypeStruct((lat_rows * tracers, lanes), BF16),
        ),
        in_specs=[VMEM] * 3,
        out_specs=(VMEM, VMEM),
        scratch_shapes=[
            pltpu.VMEM((lat_rows * lev, tracers * lanes), F32),
            pltpu.VMEM((group * CAPACITY * SLOTS, lanes), F32),
            pltpu.VMEM((lat_rows * lev, group * CAPACITY * SLOTS), BF16),
            pltpu.VMEM((group * CAPACITY * SLOTS, tracers * lanes), BF16),
            pltpu.VMEM((lat_rows * tracers, lanes), F32),
        ],
        compiler_params=pltpu.CompilerParams(**big),
        name="forcing",
    )(received, state, surface)

    smoothed = pl.pallas_call(
        functools.partial(smooth_kernel, tracers, lat_rows),
        out_shape=jax.ShapeDtypeStruct((tracers, lat_rows, lanes), F32),
        in_specs=[VMEM] * 3,
        out_specs=VMEM,
        scratch_shapes=[
            pltpu.VMEM((nlon, lat_rows * tracers, lanes), BF16),
            pltpu.VMEM((nlat, lat_rows * tracers, lanes), BF16),
            pltpu.VMEM((lat_rows * tracers, lanes), BF16),
            pltpu.SemaphoreType.DMA((nlon,)),
            pltpu.SemaphoreType.DMA((nlon,)),
            pltpu.SemaphoreType.DMA((nlat,)),
            pltpu.SemaphoreType.DMA((nlat,)),
        ],
        compiler_params=pltpu.CompilerParams(collective_id=1, has_side_effects=True, **big),
        name="smooth",
    )(low, lon_matrix, lat_matrix)
    return adjoint.reshape(adjoint_in.shape), smoothed


def solution(mesh):
    placed = (
        P(None, None, "lat", "lon"),
        P(None, None, None, "lat", "lon"),
        P(None, None, "lat", "lon"),
        P(),
        P(None, ("lat", "lon")),
        P(None, ("lat", "lon")),
        P(("lat", "lon")),
        P(("lat", "lon"), None),
        P(("lat", "lon")),
        P(),
        P("lon", None),
    )
    return jax.shard_map(
        shards,
        mesh=mesh,
        in_specs=placed,
        out_specs=(P(None, None, "lat", "lon"), P(None, "lat", "lon")),
        check_vma=False,
    )
```

```python
import functools

import jax
import jax.numpy as jnp
from jax import lax
from jax.experimental import pallas as pl
from jax.experimental.pallas import tpu as pltpu
from jax.sharding import PartitionSpec as P

STEPS = 4
CAPACITY = 6
SLOTS = 8
CHAINS = 2
MESH = pl.DeviceIdType.MESH
F32 = jnp.float32
BF16 = jnp.bfloat16
VMEM = pl.BlockSpec(memory_space=pltpu.VMEM)
SMEM = pl.BlockSpec(memory_space=pltpu.SMEM)


def padded(levels):
    return -(-levels // 16) * 16


def pack_kernel(levels, tracers, devices, w_ref, r_ref, c_ref, owner_ref, count_ref, out_ref, feat, rows, seen):
    blocks = owner_ref.shape[0]
    lanes = 128
    per_chunk = lanes // SLOTS
    feat[0:levels, :] = w_ref[...].astype(F32)
    feat[levels : levels + tracers, :] = r_ref[...].astype(F32)
    cell = c_ref[...]
    feat[levels + tracers : levels + tracers + 1, :] = (cell // lanes).astype(F32)
    feat[levels + tracers + 1 : levels + tracers + 2, :] = (cell % lanes).astype(F32)
    rows[...] = jnp.zeros_like(rows)

    @pl.loop(0, devices)
    def _(d):
        seen[d] = 0

    slot = lax.broadcasted_iota(jnp.int32, (SLOTS, lanes), 0)

    @pl.loop(0, blocks // per_chunk)
    def _(chunk):
        at = pl.multiple_of(chunk * lanes, lanes)
        turned = feat[:, pl.ds(at, lanes)].T
        for i in range(per_chunk):
            b = chunk * per_chunk + i
            owner = owner_ref[b]
            rank = seen[owner]
            seen[owner] = rank + 1
            place = pl.multiple_of((owner * CAPACITY + rank) * SLOTS, SLOTS)
            block = turned[i * SLOTS : (i + 1) * SLOTS, :]
            rows[pl.ds(place, SLOTS), :] = jnp.where(slot < count_ref[b], block, 0.0)

    width = levels + tracers + 2
    spare = lanes - width
    lane = lax.broadcasted_iota(jnp.int32, (SLOTS, lanes), 1)

    @pl.loop(0, devices, unroll=4)
    def _(d):
        base = d * (CAPACITY * SLOTS)
        got = [rows[pl.ds(pl.multiple_of(base + i * SLOTS, SLOTS), SLOTS), :] for i in range(CAPACITY)]
        pieces = []
        for i in range(4):
            extra = got[4 + i // 2]
            shift = width if i % 2 == 0 else width - spare
            pieces.append(jnp.where(lane < width, got[i], pltpu.roll(extra, shift, 1)))
        out_ref[d] = jnp.concatenate(pieces, axis=0).astype(BF16)


def exchange_kernel(
    tracers, levels, lat_rows, group,
    adj_ref, frac_ref, prof_ref, ker_ref, packed_ref, lonm_ref, latm_ref,
    out_ref, smooth_ref,
    state, surf_ref, mixed, fracs, profs, square,
    lat_send, lat_recv, lon_send, lon_recv,
    lat_ss, lat_rs, lon_ss, lon_rs,
    got, acc, slots, lhs, rhs, flat, low_ref, own_ref, lon_got, lat_got,
    all_ss, all_rs, ss_lon, rs_lon, ss_lat, rs_lat,
):
    lanes = 128
    lev = padded(levels)
    rows = levels * lat_rows
    lat, lon = lax.axis_index("lat"), lax.axis_index("lon")
    nlat, nlon = lax.axis_size("lat"), lax.axis_size("lon")
    up, down = lax.rem(lat + 1, nlat), lax.rem(lat + nlat - 1, nlat)
    east, west = lax.rem(lon + 1, nlon), lax.rem(lon + nlon - 1, nlon)
    devices = nlat * nlon
    me = lat * nlon + lon
    barrier = pltpu.get_barrier_semaphore()

    def place(d):
        to = lax.rem(me + d, devices)
        return to, {"lat": to // nlon, "lon": lax.rem(to, nlon)}

    @pl.loop(1, devices)
    def _(d):
        pl.semaphore_signal(barrier, inc=1, device_id=place(d)[1], device_id_type=MESH)

    @pl.when(lat == 0)
    def _():
        for n in range(STEPS):
            for c in range(CHAINS):
                lat_recv[n, c, 0] = jnp.zeros((lev, tracers // CHAINS * lanes), BF16)

    @pl.when(lat == nlat - 1)
    def _():
        for n in range(STEPS):
            for c in range(CHAINS):
                lat_recv[n, c, 1] = jnp.zeros((lev, tracers // CHAINS * lanes), BF16)

    square[...] = jnp.zeros_like(square)
    square[0:levels, 0:levels] = ker_ref[...].astype(F32)
    turned = square[...].T[0:lev, 0:lev].astype(BF16)
    pad = lev * lat_rows - rows
    for i in range(2):
        profs[i, 0:rows, :] = prof_ref[i * rows : (i + 1) * rows, :].astype(F32)
        profs[i, rows : rows + pad, :] = jnp.zeros((pad, lanes), F32)
    for f in range(4):
        fracs[f, rows : rows + pad, :] = jnp.zeros((pad, lanes), F32)
    for y in range(lat_rows):
        state[y, levels:lev, :] = jnp.zeros((lev - levels, tracers * lanes), F32)
        for t in range(tracers):
            state[y, 0:levels, t * lanes : (t + 1) * lanes] = adj_ref[pl.ds(t * rows + y, levels, stride=lat_rows), :]
    surf_ref[...] = jnp.zeros_like(surf_ref)
    acc[...] = jnp.zeros_like(acc)
    pl.semaphore_wait(barrier, devices - 1)

    def all_copy(d):
        to, where = place(d)
        return pltpu.make_async_remote_copy(
            src_ref=packed_ref.at[to], dst_ref=got.at[d], send_sem=all_ss.at[d], recv_sem=all_rs.at[d],
            device_id=where, device_id_type=MESH,
        )

    def send_all():
        @pl.loop(1, devices)
        def _(d):
            all_copy(d).start()

    got[0] = packed_ref[me]

    lane = lax.broadcasted_iota(jnp.int32, (lev, lanes), 1)
    half = lev // 2
    lane_half = lax.broadcasted_iota(jnp.int32, (half, lanes), 1)
    each = tracers // CHAINS
    wide = each * lanes

    def lat_copy(i, c, side):
        return pltpu.make_async_remote_copy(
            src_ref=lat_send.at[i, c, side],
            dst_ref=lat_recv.at[i, c, 1 - side],
            send_sem=lat_ss.at[i, c, side],
            recv_sem=lat_rs.at[i, c, 1 - side],
            device_id={"lat": up if side else down},
            device_id_type=MESH,
        )

    def lon_copy(i, c, side):
        return pltpu.make_async_remote_copy(
            src_ref=lon_send.at[i, c, side],
            dst_ref=lon_recv.at[i, c, 1 - side],
            send_sem=lon_ss.at[i, c, side],
            recv_sem=lon_rs.at[i, c, 1 - side],
            device_id={"lon": east if side else west},
            device_id_type=MESH,
        )

    def mix(i, c):
        columns = [jnp.zeros((lev, lanes), F32), jnp.zeros((lev, lanes), F32)]
        order = [0, lat_rows - 1] + list(range(1, lat_rows - 1))
        cs = slice(c * wide, (c + 1) * wide)
        for y in order:
            entrain = profs[0, pl.ds(y, lev, stride=lat_rows), :]
            detrain = profs[1, pl.ds(y, lev, stride=lat_rows), :]
            before = state[y, :, cs]
            lowered = (jnp.concatenate([detrain] * each, axis=1) * before).astype(BF16)
            mixing = jnp.dot(turned, lowered, preferred_element_type=F32)
            after = before + jnp.concatenate([entrain] * each, axis=1) * mixing
            mixed[y, :, cs] = after
            if y == 0:
                lat_send[i, c, 0] = after.astype(BF16)

                @pl.when(lat > 0)
                def _():
                    lat_copy(i, c, 0).start()

            if y == lat_rows - 1:
                lat_send[i, c, 1] = after.astype(BF16)

                @pl.when(lat < nlat - 1)
                def _():
                    lat_copy(i, c, 1).start()

            for t in range(each):
                at = y * each + t
                tile = after[:, t * lanes : (t + 1) * lanes]
                west_edge = tile if at == 0 else pltpu.roll(tile, at, 1)
                columns[0] = jnp.where(lane == at, west_edge, columns[0])
                columns[1] = jnp.where(lane == at, pltpu.roll(tile, at + 1, 1), columns[1])
        for side in range(2):
            lon_send[i, c, side] = columns[side].astype(BF16)
            lon_copy(i, c, side).start()

    def advance(i, c, y):
        for h in range(2):
            ks = slice(h * half, (h + 1) * half)
            f = [fracs[j, pl.ds(h * half * lat_rows + y, half, stride=lat_rows), :] for j in range(4)]
            remain = 1.0 - f[0] - f[1] - f[2] - f[3]
            from_west = lon_recv[i, c, 0].astype(F32)[ks]
            from_east = lon_recv[i, c, 1].astype(F32)[ks]
            for t in range(each):
                ts = slice(c * wide + t * lanes, c * wide + (t + 1) * lanes)
                own = slice(t * lanes, (t + 1) * lanes)
                at = y * each + t
                here = mixed[y, ks, ts]
                side_e = jnp.where(
                    lane_half == lanes - 1,
                    jnp.broadcast_to(from_east[:, at : at + 1], (half, lanes)),
                    pltpu.roll(here, lanes - 1, 1),
                )
                side_w = jnp.where(
                    lane_half == 0,
                    jnp.broadcast_to(from_west[:, at : at + 1], (half, lanes)),
                    pltpu.roll(here, 1, 1),
                )
                if y == lat_rows - 1:
                    north = lat_recv[i, c, 1, :, own].astype(F32)[ks]
                else:
                    north = mixed[y + 1, ks, ts]
                if y == 0:
                    south = lat_recv[i, c, 0, :, own].astype(F32)[ks]
                else:
                    south = mixed[y - 1, ks, ts]
                state[y, ks, ts] = remain * here + f[0] * side_e + f[1] * side_w + f[2] * north + f[3] * south

    def land(i, c):
        lon_copy(i, c, 0).wait_recv()
        lon_copy(i, c, 1).wait_recv()
        for y in range(1, lat_rows - 1):
            advance(i, c, y)

        @pl.when(lat < nlat - 1)
        def _():
            lat_copy(i, c, 0).wait_recv()

        @pl.when(lat > 0)
        def _():
            lat_copy(i, c, 1).wait_recv()

        advance(i, c, 0)
        advance(i, c, lat_rows - 1)

    width = levels + tracers + 2
    spare = lanes - width
    size = CAPACITY * SLOTS
    lane8 = lax.broadcasted_iota(jnp.int32, (SLOTS, lanes), 1)
    lane16 = lax.broadcasted_iota(jnp.int32, (16, lanes), 1).astype(F32)

    def force(g):
        for p in range(group):
            block = got[g * group + p].astype(F32)
            quarter = [block[q * SLOTS : (q + 1) * SLOTS] for q in range(4)]
            for q in range(4):
                slots[p * size + q * SLOTS : p * size + (q + 1) * SLOTS, :] = quarter[q]
            for q in range(2):
                low = pltpu.roll(quarter[2 * q], lanes - width, 1)
                high = pltpu.roll(quarter[2 * q + 1], lanes - width + spare, 1)
                at = p * size + (4 + q) * SLOTS
                slots[at : at + SLOTS, :] = jnp.where(lane8 < spare, low, high)
        for c in range(group * size // lanes):
            flipped = slots[c * lanes : (c + 1) * lanes, :].T
            weights = flipped[0:lev, :]
            row = flipped[levels + tracers : levels + tracers + 1, :]
            for y in range(lat_rows):
                lhs[y * lev : (y + 1) * lev, c * lanes : (c + 1) * lanes] = jnp.where(row == y, weights, 0.0).astype(BF16)
        for q in range(group * size // 16):
            here = slots[q * 16 : (q + 1) * 16, :]
            col = jnp.broadcast_to(here[:, width - 1 : width], (16, lanes)) == lane16
            for t in range(tracers):
                value = jnp.broadcast_to(here[:, levels + t : levels + t + 1], (16, lanes))
                rhs[q * 16 : (q + 1) * 16, t * lanes : (t + 1) * lanes] = jnp.where(col, value, 0.0).astype(BF16)
        acc[...] += jnp.dot(lhs[...], rhs[...], preferred_element_type=F32)

    def fill(g):
        @pl.loop(0, group)
        def _(p):
            @pl.when(g * group + p > 0)
            def _():
                all_copy(g * group + p).wait_recv()

        force(g)

    groups = devices // group
    per_wait = groups // (2 * CHAINS)

    mix(0, 0)
    send_all()
    for c in range(1, CHAINS):
        mix(0, c)

    def step(i, _):
        n = STEPS - 1 - i
        for f in range(4):
            at = pl.multiple_of((n * 4 + f) * rows, 8)
            fracs[f, 0:rows, :] = frac_ref[pl.ds(at, rows), :].astype(F32)
        for c in range(CHAINS):
            cs = slice(c * wide, (c + 1) * wide)

            @pl.when(i >= STEPS - 2)
            def _():
                for q in range(per_wait):
                    fill(((i - (STEPS - 2)) * CHAINS + c) * per_wait + q)

            land(i, c)

            @pl.when(i < STEPS - 1)
            def _():
                for y in range(lat_rows):
                    surf_ref[y, :, cs] += state[y, 0:8, cs]
                mix(i + 1, c)

        return 0

    lax.fori_loop(0, STEPS, step, 0)
    brows = tracers * lat_rows
    for y in range(lat_rows):
        for t in range(tracers):
            ts = slice(t * lanes, (t + 1) * lanes)
            at = y * tracers + t
            last = state[y, 0:1, ts] + acc[y * lev : y * lev + 1, ts]
            flat[at : at + 1, :] = surf_ref[y, 0:1, ts] + last
    low_ref[...] = flat[...].astype(BF16)

    def band_copy(d):
        return pltpu.make_async_remote_copy(
            src_ref=low_ref, dst_ref=lon_got.at[d], send_sem=ss_lon.at[d], recv_sem=rs_lon.at[d],
            device_id={"lon": lax.rem(lon + d, nlon)}, device_id_type=MESH,
        )

    def cross_copy(d):
        return pltpu.make_async_remote_copy(
            src_ref=own_ref, dst_ref=lat_got.at[d], send_sem=ss_lat.at[d], recv_sem=rs_lat.at[d],
            device_id={"lat": lax.rem(lat + d, nlat)}, device_id_type=MESH,
        )

    for d in range(1, nlon):
        band_copy(d).start()

    for y in range(lat_rows):
        for t in range(tracers):
            ts = slice(t * lanes, (t + 1) * lanes)
            full = state[y, :, ts] + acc[y * lev : (y + 1) * lev, ts]
            out_ref[pl.ds(t * rows + y, levels, stride=lat_rows), :] = full[0:levels]

    nrow = latm_ref.shape[0]
    pick = lax.broadcasted_iota(jnp.int32, (brows, nrow), 1) == lat * lat_rows + lax.broadcasted_iota(
        jnp.int32, (brows, nrow), 0
    ) % lat_rows
    own_rows = jnp.dot(jnp.where(pick, 1.0, 0.0).astype(BF16), latm_ref[...], preferred_element_type=F32).astype(BF16)
    spread = lax.broadcasted_iota(jnp.int32, (nrow, nrow * tracers), 0) == lax.broadcasted_iota(
        jnp.int32, (nrow, nrow * tracers), 1
    ) // tracers
    wide = jnp.dot(own_rows, jnp.where(spread, 1.0, 0.0).astype(BF16), preferred_element_type=F32)
    same = lax.broadcasted_iota(jnp.int32, (brows, nrow * tracers), 0) // lat_rows == lax.broadcasted_iota(
        jnp.int32, (brows, nrow * tracers), 1
    ) % tracers
    wide = jnp.where(same, wide, 0.0)

    contract = (((1,), (1,)), ((), ()))

    def part(d, block):
        source = lax.rem(lon - d + nlon, nlon)
        matrix = lonm_ref[:, pl.ds(pl.multiple_of(source * lanes, lanes), lanes)]
        return lax.dot_general(block, matrix, contract, preferred_element_type=F32)

    total = part(0, low_ref[...])
    for d in range(1, nlon):
        band_copy(d).wait_recv()
        total += part(d, lon_got[d])
    own_ref[...] = total.astype(BF16)
    for d in range(1, nlat):
        cross_copy(d).start()
    lat_got[0] = own_ref[...]
    blocks = []
    for d in range(nlat):
        if d:
            cross_copy(d).wait_recv()
        blocks.append(lat_got[d])
    gathered = jnp.concatenate(blocks, axis=0)
    turned = pltpu.roll(wide, (nlat - 1 - lat) * brows, 1)
    reordered = jnp.concatenate(
        [turned[:, (nlat - 1 - d) * brows : (nlat - d) * brows] for d in range(nlat)], axis=1
    ).astype(BF16)
    smoothed = jnp.dot(reordered, gathered, preferred_element_type=F32)
    smooth_ref[...] = smoothed.reshape(smooth_ref.shape)
    for d in range(1, nlon):
        band_copy(d).wait_send()
    for d in range(1, nlat):
        cross_copy(d).wait_send()
    for i in range(STEPS):
        for c in range(CHAINS):
            for side in range(2):
                lon_copy(i, c, side).wait_send()

            @pl.when(lat > 0)
            def _():
                lat_copy(i, c, 0).wait_send()

            @pl.when(lat < nlat - 1)
            def _():
                lat_copy(i, c, 1).wait_send()

    @pl.loop(1, devices)
    def _(d):
        all_copy(d).wait_send()


def shards(
    adjoint_in, fractions, profiles, kernel, obs_weights, obs_resid, obs_cols, obs_owner, obs_count, lat_matrix, lon_matrix
):
    tracers, levels, lat_rows, lanes = adjoint_in.shape
    lev = padded(levels)
    nlat, nlon = lax.axis_size("lat"), lax.axis_size("lon")
    devices = nlat * nlon
    blocks = obs_count.shape[0]
    nslots = blocks * SLOTS
    big = dict(vmem_limit_bytes=60 << 20)

    packed = pl.pallas_call(
        functools.partial(pack_kernel, levels, tracers, devices),
        out_shape=jax.ShapeDtypeStruct((devices, 4 * SLOTS, lanes), BF16),
        in_specs=[VMEM, VMEM, VMEM, SMEM, SMEM],
        out_specs=VMEM,
        scratch_shapes=[
            pltpu.VMEM((lanes, nslots), F32),
            pltpu.VMEM((devices * CAPACITY * SLOTS, lanes), F32),
            pltpu.SMEM((devices,), jnp.int32),
        ],
        compiler_params=pltpu.CompilerParams(**big),
        name="pack",
    )(obs_weights, obs_resid, obs_cols.reshape(1, nslots), obs_owner.reshape(blocks), obs_count)
    rows = levels * lat_rows
    group = min(16, devices)
    each = tracers // CHAINS
    size = CAPACITY * SLOTS
    adjoint, smoothed = pl.pallas_call(
        functools.partial(exchange_kernel, tracers, levels, lat_rows, group),
        out_shape=(
            jax.ShapeDtypeStruct((tracers * rows, lanes), F32),
            jax.ShapeDtypeStruct((tracers, lat_rows, lanes), F32),
        ),
        in_specs=[VMEM] * 7,
        out_specs=(VMEM, VMEM),
        scratch_shapes=[
            pltpu.VMEM((lat_rows, lev, tracers * lanes), F32),
            pltpu.VMEM((lat_rows, 8, tracers * lanes), F32),
            pltpu.VMEM((lat_rows, lev, tracers * lanes), F32),
            pltpu.VMEM((4, lev * lat_rows, lanes), F32),
            pltpu.VMEM((2, lev * lat_rows, lanes), F32),
            pltpu.VMEM((lanes, lanes), F32),
            pltpu.VMEM((STEPS, CHAINS, 2, lev, each * lanes), BF16),
            pltpu.VMEM((STEPS, CHAINS, 2, lev, each * lanes), BF16),
            pltpu.VMEM((STEPS, CHAINS, 2, lev, lanes), BF16),
            pltpu.VMEM((STEPS, CHAINS, 2, lev, lanes), BF16),
            pltpu.SemaphoreType.DMA((STEPS, CHAINS, 2)),
            pltpu.SemaphoreType.DMA((STEPS, CHAINS, 2)),
            pltpu.SemaphoreType.DMA((STEPS, CHAINS, 2)),
            pltpu.SemaphoreType.DMA((STEPS, CHAINS, 2)),
            pltpu.VMEM((devices, 4 * SLOTS, lanes), BF16),
            pltpu.VMEM((lat_rows * lev, tracers * lanes), F32),
            pltpu.VMEM((group * size, lanes), F32),
            pltpu.VMEM((lat_rows * lev, group * size), BF16),
            pltpu.VMEM((group * size, tracers * lanes), BF16),
            pltpu.VMEM((lat_rows * tracers, lanes), F32),
            pltpu.VMEM((lat_rows * tracers, lanes), BF16),
            pltpu.VMEM((lat_rows * tracers, lanes), BF16),
            pltpu.VMEM((nlon, lat_rows * tracers, lanes), BF16),
            pltpu.VMEM((nlat, lat_rows * tracers, lanes), BF16),
            pltpu.SemaphoreType.DMA((devices,)),
            pltpu.SemaphoreType.DMA((devices,)),
            pltpu.SemaphoreType.DMA((nlon,)),
            pltpu.SemaphoreType.DMA((nlon,)),
            pltpu.SemaphoreType.DMA((nlat,)),
            pltpu.SemaphoreType.DMA((nlat,)),
        ],
        compiler_params=pltpu.CompilerParams(collective_id=0, has_side_effects=True, **big),
        name="exchange",
    )(
        adjoint_in.reshape(tracers * rows, lanes),
        fractions.reshape(STEPS * 4 * rows, lanes),
        profiles.reshape(2 * rows, lanes),
        kernel,
        packed,
        lon_matrix,
        lat_matrix,
    )
    return adjoint.reshape(adjoint_in.shape), smoothed


def solution(mesh):
    placed = (
        P(None, None, "lat", "lon"),
        P(None, None, None, "lat", "lon"),
        P(None, None, "lat", "lon"),
        P(),
        P(None, ("lat", "lon")),
        P(None, ("lat", "lon")),
        P(("lat", "lon")),
        P(("lat", "lon"), None),
        P(("lat", "lon")),
        P(),
        P("lon", None),
    )
    return jax.shard_map(
        shards,
        mesh=mesh,
        in_specs=placed,
        out_specs=(P(None, None, "lat", "lon"), P(None, "lat", "lon")),
        check_vma=False,
    )
```

```python
import functools

import jax
import jax.numpy as jnp
from jax import lax
from jax.experimental import pallas as pl
from jax.experimental.pallas import tpu as pltpu
from jax.sharding import PartitionSpec as P

STEPS = 4
CAPACITY = 6
SLOTS = 8
CHAINS = 2
SEND_NUM = 2
USE_FROM = 1
USE_NUM, USE_DEN = 4, 3
MESH = pl.DeviceIdType.MESH
LOGICAL = pl.DeviceIdType.LOGICAL
F32 = jnp.float32
BF16 = jnp.bfloat16
VMEM = pl.BlockSpec(memory_space=pltpu.VMEM)
SMEM = pl.BlockSpec(memory_space=pltpu.SMEM)


def padded(levels):
    return -(-levels // 16) * 16


def exchange_kernel(
    tracers, levels, lat_rows, group,
    adj_ref, frac_ref, prof_ref, ker_ref, w_ref, r_ref, cell_ref, owner_ref, count_ref, lonm_ref, latm_ref,
    out_ref, smooth_ref,
    state, surf_ref, mixed, fracs, profs, square,
    lat_send, lat_recv, lon_send, lon_recv,
    lat_ss, lat_rs, lon_ss, lon_rs,
    feat, block_rows, table_v, table, table_sem, packed_ref,
    got, acc, slots, lhs, rhs, flat, low_ref, own_ref, lon_got, lat_got,
    all_ss, all_rs, ss_lon, rs_lon, ss_lat, rs_lat,
):
    lanes = 128
    lev = padded(levels)
    rows = levels * lat_rows
    lat, lon = lax.axis_index("lat"), lax.axis_index("lon")
    nlat, nlon = lax.axis_size("lat"), lax.axis_size("lon")
    up, down = lax.rem(lat + 1, nlat), lax.rem(lat + nlat - 1, nlat)
    east, west = lax.rem(lon + 1, nlon), lax.rem(lon + nlon - 1, nlon)
    devices = nlat * nlon
    me = lat * nlon + lon
    barrier = pltpu.get_barrier_semaphore()

    def place(d):
        to = me + d
        return jnp.where(to < devices, to, to - devices)

    @pl.loop(1, devices)
    def _(d):
        pl.semaphore_signal(barrier, inc=1, device_id=place(d), device_id_type=LOGICAL)

    @pl.when(lat == 0)
    def _():
        for n in range(STEPS):
            for c in range(CHAINS):
                lat_recv[n, c, 0] = jnp.zeros((lev, tracers // CHAINS * lanes), BF16)

    @pl.when(lat == nlat - 1)
    def _():
        for n in range(STEPS):
            for c in range(CHAINS):
                lat_recv[n, c, 1] = jnp.zeros((lev, tracers // CHAINS * lanes), BF16)

    square[...] = jnp.zeros_like(square)
    square[0:levels, 0:levels] = ker_ref[...].astype(F32)
    turned = square[...].T[0:lev, 0:lev].astype(BF16)
    pad = lev * lat_rows - rows
    for i in range(2):
        profs[i, 0:rows, :] = prof_ref[i * rows : (i + 1) * rows, :].astype(F32)
        profs[i, rows : rows + pad, :] = jnp.zeros((pad, lanes), F32)
    for f in range(4):
        fracs[f, rows : rows + pad, :] = jnp.zeros((pad, lanes), F32)
    for y in range(lat_rows):
        state[y, levels:lev, :] = jnp.zeros((lev - levels, tracers * lanes), F32)
        for t in range(tracers):
            state[y, 0:levels, t * lanes : (t + 1) * lanes] = adj_ref[pl.ds(t * rows + y, levels, stride=lat_rows), :]
    surf_ref[...] = jnp.zeros_like(surf_ref)
    acc[...] = jnp.zeros_like(acc)

    blocks = owner_ref.shape[1]
    owner_row = owner_ref[...]
    parts = [owner_row[:, j * lanes : (j + 1) * lanes] for j in range(blocks // lanes)]
    owner_col = jnp.concatenate([jnp.broadcast_to(p, (lanes, lanes)).T for p in parts], axis=0)
    number = lax.broadcasted_iota(jnp.int32, (blocks, lanes), 0)
    across = lax.broadcasted_iota(jnp.int32, (blocks, lanes), 1)
    earlier = jnp.zeros((blocks, lanes), jnp.int32)
    for j, p in enumerate(parts):
        earlier += jnp.where((owner_col == p) & (across + j * lanes < number), 1, 0)
    rank = jnp.sum(earlier, axis=1, keepdims=True)
    mine = jnp.where(owner_col == across, jnp.broadcast_to(rank, (blocks, lanes)), CAPACITY)
    behind = number - blocks
    for k in range(CAPACITY):
        found = jnp.sum(jnp.where(mine == k, behind, 0), axis=0, keepdims=True) + blocks
        table_v[k : k + 1, :] = found
    table_v[CAPACITY:8, :] = jnp.zeros((8 - CAPACITY, lanes), jnp.int32)
    to_scalar = pltpu.make_async_copy(table_v, table, table_sem)
    to_scalar.start()

    width = levels + tracers + 2
    spare = lanes - width
    nslots = blocks * SLOTS
    feat[levels // 8 * 8 :, :] = jnp.zeros((lanes - levels // 8 * 8, nslots), F32)
    feat[0:levels, :] = w_ref[...].astype(F32)
    feat[levels : levels + tracers, :] = r_ref[...].astype(F32)
    cell = cell_ref[...]
    feat[width - 2 : width - 1, :] = lax.shift_right_logical(cell, 7).astype(F32)
    feat[width - 1 : width, :] = (cell & (lanes - 1)).astype(F32)
    block_rows[blocks] = jnp.zeros((SLOTS, lanes), F32)
    per_tile = lanes // SLOTS

    @pl.loop(0, nslots // lanes, unroll=2)
    def _(c):
        at = pl.multiple_of(c * lanes, lanes)
        block_rows[pl.ds(c * per_tile, per_tile)] = feat[:, pl.ds(at, lanes)].T.reshape(per_tile, SLOTS, lanes)

    to_scalar.wait()
    slot_of = lax.broadcasted_iota(jnp.int32, (SLOTS, lanes), 0)
    lane8 = lax.broadcasted_iota(jnp.int32, (SLOTS, lanes), 1)

    def pack(to):
        six = []
        for k in range(CAPACITY):
            b = table[k, to]
            six.append(jnp.where(slot_of < count_ref[b], block_rows[b], 0.0))
        pieces = []
        for q in range(4):
            extra = pltpu.roll(six[4 + q // 2], width if q % 2 == 0 else width - spare, 1)
            pieces.append(jnp.where(lane8 < width, six[q], extra))
        return jnp.concatenate(pieces, axis=0).astype(BF16)

    pl.semaphore_wait(barrier, devices - 1)

    def all_copy(d):
        to = place(d)
        return pltpu.make_async_remote_copy(
            src_ref=packed_ref.at[to], dst_ref=got.at[d - 1], send_sem=all_ss, recv_sem=all_rs.at[(d - 1) // group],
            device_id=to, device_id_type=LOGICAL,
        )

    def all_wait(g, count):
        part = got.at[pl.ds(g * group, count)]
        return pltpu.make_async_remote_copy(
            src_ref=part, dst_ref=part, send_sem=all_ss, recv_sem=all_rs.at[g], device_id=me, device_id_type=LOGICAL
        )

    groups = devices // group

    def send_some(slot):
        @pl.loop(sent(slot) * group, sent(slot + 1) * group)
        def _(d):
            @pl.when(d < devices - 1)
            def _():
                to = place(d + 1)
                packed_ref[to] = pack(to)

        @pl.loop(sent(slot) * group, sent(slot + 1) * group)
        def _(d):
            @pl.when(d < devices - 1)
            def _():
                all_copy(d + 1).start()

    def sent(slot):
        return jnp.minimum(groups, slot * SEND_NUM)

    def used(slot):
        return jnp.minimum(groups, jnp.maximum(0, (slot - USE_FROM) * USE_NUM // USE_DEN))

    got[devices - 1] = pack(me)

    lane = lax.broadcasted_iota(jnp.int32, (lev, lanes), 1)
    half = lev // 2
    lane_half = lax.broadcasted_iota(jnp.int32, (half, lanes), 1)
    each = tracers // CHAINS
    wide = each * lanes

    def lat_copy(i, c, side):
        return pltpu.make_async_remote_copy(
            src_ref=lat_send.at[i, c, side],
            dst_ref=lat_recv.at[i, c, 1 - side],
            send_sem=lat_ss.at[i, c, side],
            recv_sem=lat_rs.at[i, c, 1 - side],
            device_id={"lat": up if side else down},
            device_id_type=MESH,
        )

    def lon_copy(i, c, side):
        return pltpu.make_async_remote_copy(
            src_ref=lon_send.at[i, c, side],
            dst_ref=lon_recv.at[i, c, 1 - side],
            send_sem=lon_ss.at[i, c, side],
            recv_sem=lon_rs.at[i, c, 1 - side],
            device_id={"lon": east if side else west},
            device_id_type=MESH,
        )

    def mix(i, c):
        columns = [jnp.zeros((lev, lanes), F32), jnp.zeros((lev, lanes), F32)]
        order = [0, lat_rows - 1] + list(range(1, lat_rows - 1))
        cs = slice(c * wide, (c + 1) * wide)
        for y in order:
            entrain = profs[0, pl.ds(y, lev, stride=lat_rows), :]
            detrain = profs[1, pl.ds(y, lev, stride=lat_rows), :]
            before = state[y, :, cs]
            lowered = (jnp.concatenate([detrain] * each, axis=1) * before).astype(BF16)
            mixing = jnp.dot(turned, lowered, preferred_element_type=F32)
            after = before + jnp.concatenate([entrain] * each, axis=1) * mixing
            mixed[y, :, cs] = after
            if y == 0:
                lat_send[i, c, 0] = after.astype(BF16)

                @pl.when(lat > 0)
                def _():
                    lat_copy(i, c, 0).start()

            if y == lat_rows - 1:
                lat_send[i, c, 1] = after.astype(BF16)

                @pl.when(lat < nlat - 1)
                def _():
                    lat_copy(i, c, 1).start()

            for t in range(each):
                at = y * each + t
                tile = after[:, t * lanes : (t + 1) * lanes]
                west_edge = tile if at == 0 else pltpu.roll(tile, at, 1)
                columns[0] = jnp.where(lane == at, west_edge, columns[0])
                columns[1] = jnp.where(lane == at, pltpu.roll(tile, at + 1, 1), columns[1])
        for side in range(2):
            lon_send[i, c, side] = columns[side].astype(BF16)
            lon_copy(i, c, side).start()

    def advance(i, c, y):
        for h in range(2):
            ks = slice(h * half, (h + 1) * half)
            f = [fracs[j, pl.ds(h * half * lat_rows + y, half, stride=lat_rows), :] for j in range(4)]
            remain = 1.0 - f[0] - f[1] - f[2] - f[3]
            from_west = lon_recv[i, c, 0].astype(F32)[ks]
            from_east = lon_recv[i, c, 1].astype(F32)[ks]
            for t in range(each):
                ts = slice(c * wide + t * lanes, c * wide + (t + 1) * lanes)
                own = slice(t * lanes, (t + 1) * lanes)
                at = y * each + t
                here = mixed[y, ks, ts]
                side_e = jnp.where(
                    lane_half == lanes - 1,
                    jnp.broadcast_to(from_east[:, at : at + 1], (half, lanes)),
                    pltpu.roll(here, lanes - 1, 1),
                )
                side_w = jnp.where(
                    lane_half == 0,
                    jnp.broadcast_to(from_west[:, at : at + 1], (half, lanes)),
                    pltpu.roll(here, 1, 1),
                )
                if y == lat_rows - 1:
                    north = lat_recv[i, c, 1, :, own].astype(F32)[ks]
                else:
                    north = mixed[y + 1, ks, ts]
                if y == 0:
                    south = lat_recv[i, c, 0, :, own].astype(F32)[ks]
                else:
                    south = mixed[y - 1, ks, ts]
                state[y, ks, ts] = remain * here + f[0] * side_e + f[1] * side_w + f[2] * north + f[3] * south

    def land(i, c):
        lon_copy(i, c, 0).wait_recv()
        lon_copy(i, c, 1).wait_recv()
        for y in range(1, lat_rows - 1):
            advance(i, c, y)

        @pl.when(lat < nlat - 1)
        def _():
            lat_copy(i, c, 0).wait_recv()

        @pl.when(lat > 0)
        def _():
            lat_copy(i, c, 1).wait_recv()

        advance(i, c, 0)
        advance(i, c, lat_rows - 1)

    size = CAPACITY * SLOTS
    lane16 = lax.broadcasted_iota(jnp.int32, (16, lanes), 1).astype(F32)

    def force(g):
        for p in range(group):
            block = got[g * group + p].astype(F32)
            quarter = [block[q * SLOTS : (q + 1) * SLOTS] for q in range(4)]
            for q in range(4):
                slots[p * size + q * SLOTS : p * size + (q + 1) * SLOTS, :] = quarter[q]
            for q in range(2):
                low = pltpu.roll(quarter[2 * q], lanes - width, 1)
                high = pltpu.roll(quarter[2 * q + 1], lanes - width + spare, 1)
                at = p * size + (4 + q) * SLOTS
                slots[at : at + SLOTS, :] = jnp.where(lane8 < spare, low, high)
        for c in range(group * size // lanes):
            flipped = slots[c * lanes : (c + 1) * lanes, :].T
            weights = flipped[0:lev, :]
            row = flipped[levels + tracers : levels + tracers + 1, :]
            for y in range(lat_rows):
                lhs[y * lev : (y + 1) * lev, c * lanes : (c + 1) * lanes] = jnp.where(row == y, weights, 0.0).astype(BF16)
        for q in range(group * size // 16):
            here = slots[q * 16 : (q + 1) * 16, :]
            col = jnp.broadcast_to(here[:, width - 1 : width], (16, lanes)) == lane16
            for t in range(tracers):
                value = jnp.broadcast_to(here[:, levels + t : levels + t + 1], (16, lanes))
                rhs[q * 16 : (q + 1) * 16, t * lanes : (t + 1) * lanes] = jnp.where(col, value, 0.0).astype(BF16)
        acc[...] += jnp.dot(lhs[...], rhs[...], preferred_element_type=F32)

    def fill(g):
        @pl.when(g < groups - 1)
        def _():
            all_wait(g, group).wait_recv()

        @pl.when(g == groups - 1)
        def _():
            all_wait(g, group - 1).wait_recv()

        force(g)

    for c in range(CHAINS):
        mix(0, c)
        send_some(c)

    def step(i, _):
        n = STEPS - 1 - i
        for f in range(4):
            at = pl.multiple_of((n * 4 + f) * rows, 8)
            fracs[f, 0:rows, :] = frac_ref[pl.ds(at, rows), :].astype(F32)
        for c in range(CHAINS):
            cs = slice(c * wide, (c + 1) * wide)

            slot = i * CHAINS + c
            pl.loop(used(slot - 1), used(slot))(fill)
            land(i, c)

            @pl.when(i < STEPS - 1)
            def _():
                for y in range(lat_rows):
                    surf_ref[y, :, cs] += state[y, 0:8, cs]
                mix(i + 1, c)
                send_some((i + 1) * CHAINS + c)

        return 0

    lax.fori_loop(0, STEPS, step, 0)
    brows = tracers * lat_rows
    for y in range(lat_rows):
        for t in range(tracers):
            ts = slice(t * lanes, (t + 1) * lanes)
            at = y * tracers + t
            last = state[y, 0:1, ts] + acc[y * lev : y * lev + 1, ts]
            flat[at : at + 1, :] = surf_ref[y, 0:1, ts] + last
    low_ref[...] = flat[...].astype(BF16)

    def band_copy(d):
        return pltpu.make_async_remote_copy(
            src_ref=low_ref, dst_ref=lon_got.at[d], send_sem=ss_lon.at[d], recv_sem=rs_lon.at[d],
            device_id={"lon": lax.rem(lon + d, nlon)}, device_id_type=MESH,
        )

    def cross_copy(d):
        return pltpu.make_async_remote_copy(
            src_ref=own_ref, dst_ref=lat_got.at[d], send_sem=ss_lat.at[d], recv_sem=rs_lat.at[d],
            device_id={"lat": lax.rem(lat + d, nlat)}, device_id_type=MESH,
        )

    for d in range(1, nlon):
        band_copy(d).start()

    for y in range(lat_rows):
        for t in range(tracers):
            ts = slice(t * lanes, (t + 1) * lanes)
            full = state[y, :, ts] + acc[y * lev : (y + 1) * lev, ts]
            out_ref[pl.ds(t * rows + y, levels, stride=lat_rows), :] = full[0:levels]

    nrow = latm_ref.shape[0]
    pick = lax.broadcasted_iota(jnp.int32, (brows, nrow), 1) == lat * lat_rows + lax.broadcasted_iota(
        jnp.int32, (brows, nrow), 0
    ) % lat_rows
    own_rows = jnp.dot(jnp.where(pick, 1.0, 0.0).astype(BF16), latm_ref[...], preferred_element_type=F32).astype(BF16)
    spread = lax.broadcasted_iota(jnp.int32, (nrow, nrow * tracers), 0) == lax.broadcasted_iota(
        jnp.int32, (nrow, nrow * tracers), 1
    ) // tracers
    wide = jnp.dot(own_rows, jnp.where(spread, 1.0, 0.0).astype(BF16), preferred_element_type=F32)
    same = lax.broadcasted_iota(jnp.int32, (brows, nrow * tracers), 0) // lat_rows == lax.broadcasted_iota(
        jnp.int32, (brows, nrow * tracers), 1
    ) % tracers
    wide = jnp.where(same, wide, 0.0)

    contract = (((1,), (1,)), ((), ()))

    def part(d, block):
        source = lax.rem(lon - d + nlon, nlon)
        matrix = lonm_ref[:, pl.ds(pl.multiple_of(source * lanes, lanes), lanes)]
        return lax.dot_general(block, matrix, contract, preferred_element_type=F32)

    total = part(0, low_ref[...])
    for d in range(1, nlon):
        band_copy(d).wait_recv()
        total += part(d, lon_got[d])
    own_ref[...] = total.astype(BF16)
    for d in range(1, nlat):
        cross_copy(d).start()
    lat_got[0] = own_ref[...]
    blocks = []
    for d in range(nlat):
        if d:
            cross_copy(d).wait_recv()
        blocks.append(lat_got[d])
    gathered = jnp.concatenate(blocks, axis=0)
    turned = pltpu.roll(wide, (nlat - 1 - lat) * brows, 1)
    reordered = jnp.concatenate(
        [turned[:, (nlat - 1 - d) * brows : (nlat - d) * brows] for d in range(nlat)], axis=1
    ).astype(BF16)
    smoothed = jnp.dot(reordered, gathered, preferred_element_type=F32)
    smooth_ref[...] = smoothed.reshape(smooth_ref.shape)
    for d in range(1, nlon):
        band_copy(d).wait_send()
    for d in range(1, nlat):
        cross_copy(d).wait_send()
    for i in range(STEPS):
        for c in range(CHAINS):
            for side in range(2):
                lon_copy(i, c, side).wait_send()

            @pl.when(lat > 0)
            def _():
                lat_copy(i, c, 0).wait_send()

            @pl.when(lat < nlat - 1)
            def _():
                lat_copy(i, c, 1).wait_send()

    sent_all = packed_ref.at[pl.ds(0, devices - 1)]
    pltpu.make_async_remote_copy(
        src_ref=sent_all, dst_ref=sent_all, send_sem=all_ss, recv_sem=all_rs.at[0], device_id=me, device_id_type=LOGICAL
    ).wait_send()


def shards(
    adjoint_in, fractions, profiles, kernel, obs_weights, obs_resid, obs_cols, obs_owner, obs_count, lat_matrix, lon_matrix
):
    tracers, levels, lat_rows, lanes = adjoint_in.shape
    lev = padded(levels)
    nlat, nlon = lax.axis_size("lat"), lax.axis_size("lon")
    devices = nlat * nlon
    blocks = obs_count.shape[0]
    nslots = blocks * SLOTS
    big = dict(vmem_limit_bytes=60 << 20)

    rows = levels * lat_rows
    group = min(16, devices)
    each = tracers // CHAINS
    size = CAPACITY * SLOTS
    adjoint, smoothed = pl.pallas_call(
        functools.partial(exchange_kernel, tracers, levels, lat_rows, group),
        out_shape=(
            jax.ShapeDtypeStruct((tracers * rows, lanes), F32),
            jax.ShapeDtypeStruct((tracers, lat_rows, lanes), F32),
        ),
        in_specs=[VMEM] * 8 + [SMEM] + [VMEM] * 2,
        out_specs=(VMEM, VMEM),
        scratch_shapes=[
            pltpu.VMEM((lat_rows, lev, tracers * lanes), F32),
            pltpu.VMEM((lat_rows, 8, tracers * lanes), F32),
            pltpu.VMEM((lat_rows, lev, tracers * lanes), F32),
            pltpu.VMEM((4, lev * lat_rows, lanes), F32),
            pltpu.VMEM((2, lev * lat_rows, lanes), F32),
            pltpu.VMEM((lanes, lanes), F32),
            pltpu.VMEM((STEPS, CHAINS, 2, lev, each * lanes), BF16),
            pltpu.VMEM((STEPS, CHAINS, 2, lev, each * lanes), BF16),
            pltpu.VMEM((STEPS, CHAINS, 2, lev, lanes), BF16),
            pltpu.VMEM((STEPS, CHAINS, 2, lev, lanes), BF16),
            pltpu.SemaphoreType.DMA((STEPS, CHAINS, 2)),
            pltpu.SemaphoreType.DMA((STEPS, CHAINS, 2)),
            pltpu.SemaphoreType.DMA((STEPS, CHAINS, 2)),
            pltpu.SemaphoreType.DMA((STEPS, CHAINS, 2)),
            pltpu.VMEM((lanes, nslots), F32),
            pltpu.VMEM((blocks + 1, SLOTS, lanes), F32),
            pltpu.VMEM((8, lanes), jnp.int32),
            pltpu.SMEM((8, lanes), jnp.int32),
            pltpu.SemaphoreType.DMA,
            pltpu.VMEM((devices, 4 * SLOTS, lanes), BF16),
            pltpu.VMEM((devices, 4 * SLOTS, lanes), BF16),
            pltpu.VMEM((lat_rows * lev, tracers * lanes), F32),
            pltpu.VMEM((group * size, lanes), F32),
            pltpu.VMEM((lat_rows * lev, group * size), BF16),
            pltpu.VMEM((group * size, tracers * lanes), BF16),
            pltpu.VMEM((lat_rows * tracers, lanes), F32),
            pltpu.VMEM((lat_rows * tracers, lanes), BF16),
            pltpu.VMEM((lat_rows * tracers, lanes), BF16),
            pltpu.VMEM((nlon, lat_rows * tracers, lanes), BF16),
            pltpu.VMEM((nlat, lat_rows * tracers, lanes), BF16),
            pltpu.SemaphoreType.DMA,
            pltpu.SemaphoreType.DMA((devices // group,)),
            pltpu.SemaphoreType.DMA((nlon,)),
            pltpu.SemaphoreType.DMA((nlon,)),
            pltpu.SemaphoreType.DMA((nlat,)),
            pltpu.SemaphoreType.DMA((nlat,)),
        ],
        compiler_params=pltpu.CompilerParams(collective_id=0, has_side_effects=True, **big),
        name="exchange",
    )(
        adjoint_in.reshape(tracers * rows, lanes),
        fractions.reshape(STEPS * 4 * rows, lanes),
        profiles.reshape(2 * rows, lanes),
        kernel,
        obs_weights,
        obs_resid,
        obs_cols.reshape(1, nslots),
        obs_owner.reshape(1, blocks),
        jnp.pad(obs_count, (0, lanes)),
        lon_matrix,
        lat_matrix,
    )
    return adjoint.reshape(adjoint_in.shape), smoothed


def solution(mesh):
    placed = (
        P(None, None, "lat", "lon"),
        P(None, None, None, "lat", "lon"),
        P(None, None, "lat", "lon"),
        P(),
        P(None, ("lat", "lon")),
        P(None, ("lat", "lon")),
        P(("lat", "lon")),
        P(("lat", "lon"), None),
        P(("lat", "lon")),
        P(),
        P("lon", None),
    )
    return jax.shard_map(
        shards,
        mesh=mesh,
        in_specs=placed,
        out_specs=(P(None, None, "lat", "lon"), P(None, "lat", "lon")),
        check_vma=False,
    )
```

```python
import functools

import jax
import jax.numpy as jnp
from jax import lax
from jax.experimental import pallas as pl
from jax.experimental.pallas import tpu as pltpu
from jax.sharding import PartitionSpec as P

STEPS = 4
CAPACITY = 6
SLOTS = 8
CHAINS = 2
SEND_NUM = 2
USE_FROM = 0
USE_NUM, USE_DEN = 8, 7
MESH = pl.DeviceIdType.MESH
LOGICAL = pl.DeviceIdType.LOGICAL
F32 = jnp.float32
BF16 = jnp.bfloat16
VMEM = pl.BlockSpec(memory_space=pltpu.VMEM)
SMEM = pl.BlockSpec(memory_space=pltpu.SMEM)


def padded(levels):
    return -(-levels // 16) * 16


def exchange_kernel(
    tracers, levels, lat_rows, group,
    adj_ref, frac_ref, prof_ref, ker_ref, w_ref, r_ref, cell_ref, owner_ref, count_ref, lonm_ref, latm_ref,
    out_ref, smooth_ref,
    state, surf_ref, mixed, fracs, profs, square,
    lat_send, lat_recv, lon_send, lon_recv,
    lat_ss, lat_rs, lon_ss, lon_rs,
    feat, block_rows, table_v, table, table_sem, packed_ref,
    got, acc, slots, lhs, rhs, flat, low_ref, own_ref, lon_got, lat_got, lon_turned, lat_ordered,
    all_ss, all_rs, ss_lon, rs_lon, ss_lat, rs_lat,
):
    lanes = 128
    lev = padded(levels)
    rows = levels * lat_rows
    lat, lon = lax.axis_index("lat"), lax.axis_index("lon")
    nlat, nlon = lax.axis_size("lat"), lax.axis_size("lon")
    up, down = lax.rem(lat + 1, nlat), lax.rem(lat + nlat - 1, nlat)
    east, west = lax.rem(lon + 1, nlon), lax.rem(lon + nlon - 1, nlon)
    devices = nlat * nlon
    me = lat * nlon + lon
    barrier = pltpu.get_barrier_semaphore()

    def place(d):
        to = me + d
        return jnp.where(to < devices, to, to - devices)

    @pl.loop(1, devices)
    def _(d):
        pl.semaphore_signal(barrier, inc=1, device_id=place(d), device_id_type=LOGICAL)

    @pl.when(lat == 0)
    def _():
        for n in range(STEPS):
            for c in range(CHAINS):
                lat_recv[n, c, 0] = jnp.zeros((lev, tracers // CHAINS * lanes), BF16)

    @pl.when(lat == nlat - 1)
    def _():
        for n in range(STEPS):
            for c in range(CHAINS):
                lat_recv[n, c, 1] = jnp.zeros((lev, tracers // CHAINS * lanes), BF16)

    square[...] = jnp.zeros_like(square)
    square[0:levels, 0:levels] = ker_ref[...].astype(F32)
    turned = square[...].T[0:lev, 0:lev].astype(BF16)
    pad = lev * lat_rows - rows
    for i in range(2):
        profs[i, 0:rows, :] = prof_ref[i * rows : (i + 1) * rows, :].astype(F32)
        profs[i, rows : rows + pad, :] = jnp.zeros((pad, lanes), F32)
    for f in range(4):
        fracs[f, rows : rows + pad, :] = jnp.zeros((pad, lanes), F32)
    for y in range(lat_rows):
        state[y, levels:lev, :] = jnp.zeros((lev - levels, tracers * lanes), F32)
        for t in range(tracers):
            state[y, 0:levels, t * lanes : (t + 1) * lanes] = adj_ref[pl.ds(t * rows + y, levels, stride=lat_rows), :]
    surf_ref[...] = jnp.zeros_like(surf_ref)
    acc[...] = jnp.zeros_like(acc)

    blocks = owner_ref.shape[1]
    owner_row = owner_ref[...]
    parts = [owner_row[:, j * lanes : (j + 1) * lanes] for j in range(blocks // lanes)]
    owner_col = jnp.concatenate([jnp.broadcast_to(p, (lanes, lanes)).T for p in parts], axis=0)
    number = lax.broadcasted_iota(jnp.int32, (blocks, lanes), 0)
    across = lax.broadcasted_iota(jnp.int32, (blocks, lanes), 1)
    earlier = jnp.zeros((blocks, lanes), jnp.int32)
    for j, p in enumerate(parts):
        earlier += jnp.where((owner_col == p) & (across + j * lanes < number), 1, 0)
    rank = jnp.sum(earlier, axis=1, keepdims=True)
    mine = jnp.where(owner_col == across, jnp.broadcast_to(rank, (blocks, lanes)), CAPACITY)
    count_row = count_ref[...]
    count_col = jnp.concatenate(
        [jnp.broadcast_to(count_row[:, j * lanes : (j + 1) * lanes], (lanes, lanes)).T for j in range(blocks // lanes)], axis=0
    )
    table_v[...] = jnp.zeros_like(table_v)
    for k in range(CAPACITY):
        hit = mine == k
        table_v[k : k + 1, :] = jnp.sum(jnp.where(hit, number, 0), axis=0, keepdims=True)
        table_v[8 + k : 9 + k, :] = jnp.sum(jnp.where(hit, count_col, 0), axis=0, keepdims=True)
    to_scalar = pltpu.make_async_copy(table_v, table, table_sem)
    to_scalar.start()

    width = levels + tracers + 2
    spare = lanes - width
    nslots = blocks * SLOTS
    feat[levels // 8 * 8 :, :] = jnp.zeros((lanes - levels // 8 * 8, nslots), F32)
    feat[0:levels, :] = w_ref[...].astype(F32)
    feat[levels : levels + tracers, :] = r_ref[...].astype(F32)
    cell = cell_ref[...]
    feat[width - 2 : width - 1, :] = lax.shift_right_logical(cell, 7).astype(F32)
    feat[width - 1 : width, :] = (cell & (lanes - 1)).astype(F32)
    per_tile = lanes // SLOTS

    @pl.loop(0, nslots // lanes, unroll=2)
    def _(c):
        at = pl.multiple_of(c * lanes, lanes)
        block_rows[pl.ds(c * per_tile, per_tile)] = feat[:, pl.ds(at, lanes)].T.reshape(per_tile, SLOTS, lanes)

    to_scalar.wait()
    slot_of = lax.broadcasted_iota(jnp.int32, (SLOTS, lanes), 0)
    lane8 = lax.broadcasted_iota(jnp.int32, (SLOTS, lanes), 1)

    def pack(to):
        six = []
        for k in range(CAPACITY):
            b = table[k, to]
            six.append(jnp.where(slot_of < table[8 + k, to], block_rows[b], 0.0))
        pieces = []
        for q in range(4):
            extra = pltpu.roll(six[4 + q // 2], width if q % 2 == 0 else width - spare, 1)
            pieces.append(jnp.where(lane8 < width, six[q], extra))
        return jnp.concatenate(pieces, axis=0).astype(BF16)

    pl.semaphore_wait(barrier, devices - 1)

    def all_copy(d):
        to = place(d)
        return pltpu.make_async_remote_copy(
            src_ref=packed_ref.at[to], dst_ref=got.at[d - 1], send_sem=all_ss, recv_sem=all_rs.at[(d - 1) // group],
            device_id=to, device_id_type=LOGICAL,
        )

    def all_wait(g, count):
        part = got.at[pl.ds(g * group, count)]
        return pltpu.make_async_remote_copy(
            src_ref=part, dst_ref=part, send_sem=all_ss, recv_sem=all_rs.at[g], device_id=me, device_id_type=LOGICAL
        )

    groups = devices // group

    def send_some(slot):
        @pl.loop(sent(slot), sent(slot + 1))
        def _(g):
            @pl.loop(0, group, unroll=8)
            def _(p):
                to = place(g * group + p + 1)
                packed_ref[to] = pack(to)

        @pl.loop(sent(slot) * group, sent(slot + 1) * group)
        def _(d):
            @pl.when(d < devices - 1)
            def _():
                all_copy(d + 1).start()

    def sent(slot):
        return jnp.minimum(groups, slot * SEND_NUM)

    def used(slot):
        return jnp.minimum(groups, jnp.maximum(0, (slot - USE_FROM) * USE_NUM // USE_DEN))

    got[devices - 1] = pack(me)

    lane = lax.broadcasted_iota(jnp.int32, (lev, lanes), 1)
    half = lev // 2
    lane_half = lax.broadcasted_iota(jnp.int32, (half, lanes), 1)
    each = tracers // CHAINS
    wide = each * lanes

    def lat_copy(i, c, side):
        return pltpu.make_async_remote_copy(
            src_ref=lat_send.at[i, c, side],
            dst_ref=lat_recv.at[i, c, 1 - side],
            send_sem=lat_ss.at[i, c, side],
            recv_sem=lat_rs.at[i, c, 1 - side],
            device_id={"lat": up if side else down},
            device_id_type=MESH,
        )

    def lon_copy(i, c, side):
        return pltpu.make_async_remote_copy(
            src_ref=lon_send.at[i, c, side],
            dst_ref=lon_recv.at[i, c, 1 - side],
            send_sem=lon_ss.at[i, c, side],
            recv_sem=lon_rs.at[i, c, 1 - side],
            device_id={"lon": east if side else west},
            device_id_type=MESH,
        )

    def mix(i, c):
        columns = [jnp.zeros((lev, lanes), F32), jnp.zeros((lev, lanes), F32)]
        order = [0, lat_rows - 1] + list(range(1, lat_rows - 1))
        cs = slice(c * wide, (c + 1) * wide)
        for y in order:
            entrain = profs[0, pl.ds(y, lev, stride=lat_rows), :]
            detrain = profs[1, pl.ds(y, lev, stride=lat_rows), :]
            before = state[y, :, cs]
            lowered = (jnp.concatenate([detrain] * each, axis=1) * before).astype(BF16)
            mixing = jnp.dot(turned, lowered, preferred_element_type=F32)
            after = before + jnp.concatenate([entrain] * each, axis=1) * mixing
            mixed[y, :, cs] = after
            if y == 0:
                lat_send[i, c, 0] = after.astype(BF16)

                @pl.when(lat > 0)
                def _():
                    lat_copy(i, c, 0).start()

            if y == lat_rows - 1:
                lat_send[i, c, 1] = after.astype(BF16)

                @pl.when(lat < nlat - 1)
                def _():
                    lat_copy(i, c, 1).start()

            for t in range(each):
                at = y * each + t
                tile = after[:, t * lanes : (t + 1) * lanes]
                west_edge = tile if at == 0 else pltpu.roll(tile, at, 1)
                columns[0] = jnp.where(lane == at, west_edge, columns[0])
                columns[1] = jnp.where(lane == at, pltpu.roll(tile, at + 1, 1), columns[1])
        for side in range(2):
            lon_send[i, c, side] = columns[side].astype(BF16)
            lon_copy(i, c, side).start()

    def advance(i, c, y):
        for h in range(2):
            ks = slice(h * half, (h + 1) * half)
            f = [fracs[j, pl.ds(h * half * lat_rows + y, half, stride=lat_rows), :] for j in range(4)]
            remain = 1.0 - f[0] - f[1] - f[2] - f[3]
            from_west = lon_recv[i, c, 0].astype(F32)[ks]
            from_east = lon_recv[i, c, 1].astype(F32)[ks]
            for t in range(each):
                ts = slice(c * wide + t * lanes, c * wide + (t + 1) * lanes)
                own = slice(t * lanes, (t + 1) * lanes)
                at = y * each + t
                here = mixed[y, ks, ts]
                side_e = jnp.where(
                    lane_half == lanes - 1,
                    jnp.broadcast_to(from_east[:, at : at + 1], (half, lanes)),
                    pltpu.roll(here, lanes - 1, 1),
                )
                side_w = jnp.where(
                    lane_half == 0,
                    jnp.broadcast_to(from_west[:, at : at + 1], (half, lanes)),
                    pltpu.roll(here, 1, 1),
                )
                if y == lat_rows - 1:
                    north = lat_recv[i, c, 1, :, own].astype(F32)[ks]
                else:
                    north = mixed[y + 1, ks, ts]
                if y == 0:
                    south = lat_recv[i, c, 0, :, own].astype(F32)[ks]
                else:
                    south = mixed[y - 1, ks, ts]
                state[y, ks, ts] = remain * here + f[0] * side_e + f[1] * side_w + f[2] * north + f[3] * south

    def land(i, c):
        lon_copy(i, c, 0).wait_recv()
        lon_copy(i, c, 1).wait_recv()
        for y in range(1, lat_rows - 1):
            advance(i, c, y)

        @pl.when(lat < nlat - 1)
        def _():
            lat_copy(i, c, 0).wait_recv()

        @pl.when(lat > 0)
        def _():
            lat_copy(i, c, 1).wait_recv()

        advance(i, c, 0)
        advance(i, c, lat_rows - 1)

    size = CAPACITY * SLOTS
    lane16 = lax.broadcasted_iota(jnp.int32, (16, lanes), 1).astype(F32)

    def force(g):
        for p in range(group):
            block = got[g * group + p].astype(F32)
            quarter = [block[q * SLOTS : (q + 1) * SLOTS] for q in range(4)]
            for q in range(4):
                slots[p * size + q * SLOTS : p * size + (q + 1) * SLOTS, :] = quarter[q]
            for q in range(2):
                low = pltpu.roll(quarter[2 * q], lanes - width, 1)
                high = pltpu.roll(quarter[2 * q + 1], lanes - width + spare, 1)
                at = p * size + (4 + q) * SLOTS
                slots[at : at + SLOTS, :] = jnp.where(lane8 < spare, low, high)
        for c in range(group * size // lanes):
            flipped = slots[c * lanes : (c + 1) * lanes, :].T
            weights = flipped[0:lev, :]
            row = flipped[levels + tracers : levels + tracers + 1, :]
            for y in range(lat_rows):
                lhs[y * lev : (y + 1) * lev, c * lanes : (c + 1) * lanes] = jnp.where(row == y, weights, 0.0).astype(BF16)
        for q in range(group * size // 16):
            here = slots[q * 16 : (q + 1) * 16, :]
            col = jnp.broadcast_to(here[:, width - 1 : width], (16, lanes)) == lane16
            for t in range(tracers):
                value = jnp.broadcast_to(here[:, levels + t : levels + t + 1], (16, lanes))
                rhs[q * 16 : (q + 1) * 16, t * lanes : (t + 1) * lanes] = jnp.where(col, value, 0.0).astype(BF16)
        acc[...] += jnp.dot(lhs[...], rhs[...], preferred_element_type=F32)

    def fill(g):
        @pl.when(g < groups - 1)
        def _():
            all_wait(g, group).wait_recv()

        @pl.when(g == groups - 1)
        def _():
            all_wait(g, group - 1).wait_recv()

        force(g)

    for c in range(CHAINS):
        mix(0, c)
        send_some(c)

    def matrices():
        brows = tracers * lat_rows
        nrow = latm_ref.shape[0]
        pick = lax.broadcasted_iota(jnp.int32, (brows, nrow), 1) == lat * lat_rows + lax.broadcasted_iota(
            jnp.int32, (brows, nrow), 0
        ) % lat_rows
        own_rows = jnp.dot(jnp.where(pick, 1.0, 0.0).astype(BF16), latm_ref[...], preferred_element_type=F32).astype(BF16)
        spread = lax.broadcasted_iota(jnp.int32, (nrow, nrow * tracers), 0) == lax.broadcasted_iota(
            jnp.int32, (nrow, nrow * tracers), 1
        ) // tracers
        wide = jnp.dot(own_rows, jnp.where(spread, 1.0, 0.0).astype(BF16), preferred_element_type=F32)
        same = lax.broadcasted_iota(jnp.int32, (brows, nrow * tracers), 0) // lat_rows == lax.broadcasted_iota(
            jnp.int32, (brows, nrow * tracers), 1
        ) % tracers
        wide = jnp.where(same, wide, 0.0)

        rolled = pltpu.roll(wide, (nlat - 1 - lat) * brows, 1)
        lat_ordered[...] = jnp.concatenate(
            [rolled[:, (nlat - 1 - d) * brows : (nlat - d) * brows] for d in range(nlat)], axis=1
        ).astype(BF16)

        @pl.loop(0, nlon, unroll=2)
        def _(d):
            source = lax.rem(lon - d + nlon, nlon)
            part = lonm_ref[:, pl.ds(pl.multiple_of(source * lanes, lanes), lanes)].astype(F32)
            lon_turned[pl.ds(pl.multiple_of(d * lanes, lanes), lanes), :] = part.T.astype(BF16)

    def step(i, _):
        n = STEPS - 1 - i
        for f in range(4):
            at = pl.multiple_of((n * 4 + f) * rows, 8)
            fracs[f, 0:rows, :] = frac_ref[pl.ds(at, rows), :].astype(F32)
        for c in range(CHAINS):
            cs = slice(c * wide, (c + 1) * wide)

            slot = i * CHAINS + c
            if c == 0:
                pl.when(i == 2)(matrices)
            pl.loop(used(slot - 1), used(slot))(fill)
            land(i, c)

            @pl.when(i < STEPS - 1)
            def _():
                for y in range(lat_rows):
                    surf_ref[y, :, cs] += state[y, 0:8, cs]
                mix(i + 1, c)
                send_some((i + 1) * CHAINS + c)

        return 0

    lax.fori_loop(0, STEPS, step, 0)
    brows = tracers * lat_rows
    for y in range(lat_rows):
        for t in range(tracers):
            ts = slice(t * lanes, (t + 1) * lanes)
            at = y * tracers + t
            last = state[y, 0:1, ts] + acc[y * lev : y * lev + 1, ts]
            flat[at : at + 1, :] = surf_ref[y, 0:1, ts] + last
    low_ref[...] = flat[...].astype(BF16)

    def band_copy(d):
        return pltpu.make_async_remote_copy(
            src_ref=low_ref, dst_ref=lon_got.at[d], send_sem=ss_lon.at[d], recv_sem=rs_lon.at[d],
            device_id={"lon": lax.rem(lon + d, nlon)}, device_id_type=MESH,
        )

    def cross_copy(d):
        return pltpu.make_async_remote_copy(
            src_ref=own_ref, dst_ref=lat_got.at[d], send_sem=ss_lat.at[d], recv_sem=rs_lat.at[d],
            device_id={"lat": lax.rem(lat + d, nlat)}, device_id_type=MESH,
        )

    for d in range(1, nlon):
        band_copy(d).start()

    for y in range(lat_rows):
        for t in range(tracers):
            ts = slice(t * lanes, (t + 1) * lanes)
            full = state[y, :, ts] + acc[y * lev : (y + 1) * lev, ts]
            out_ref[pl.ds(t * rows + y, levels, stride=lat_rows), :] = full[0:levels]

    lon_got[0] = low_ref[...]
    for d in range(1, nlon):
        band_copy(d).wait_recv()
    band = jnp.concatenate([lon_got[d] for d in range(nlon)], axis=1)
    own_ref[...] = jnp.dot(band, lon_turned[...], preferred_element_type=F32).astype(BF16)
    for d in range(1, nlat):
        cross_copy(d).start()
    lat_got[0] = own_ref[...]
    blocks = []
    for d in range(nlat):
        if d:
            cross_copy(d).wait_recv()
        blocks.append(lat_got[d])
    gathered = jnp.concatenate(blocks, axis=0)
    smoothed = jnp.dot(lat_ordered[...], gathered, preferred_element_type=F32)
    smooth_ref[...] = smoothed.reshape(smooth_ref.shape)
    for d in range(1, nlon):
        band_copy(d).wait_send()
    for d in range(1, nlat):
        cross_copy(d).wait_send()
    for i in range(STEPS):
        for c in range(CHAINS):
            for side in range(2):
                lon_copy(i, c, side).wait_send()

            @pl.when(lat > 0)
            def _():
                lat_copy(i, c, 0).wait_send()

            @pl.when(lat < nlat - 1)
            def _():
                lat_copy(i, c, 1).wait_send()

    sent_all = packed_ref.at[pl.ds(0, devices - 1)]
    pltpu.make_async_remote_copy(
        src_ref=sent_all, dst_ref=sent_all, send_sem=all_ss, recv_sem=all_rs.at[0], device_id=me, device_id_type=LOGICAL
    ).wait_send()


def shards(
    adjoint_in, fractions, profiles, kernel, obs_weights, obs_resid, obs_cols, obs_owner, obs_count, lat_matrix, lon_matrix
):
    tracers, levels, lat_rows, lanes = adjoint_in.shape
    lev = padded(levels)
    nlat, nlon = lax.axis_size("lat"), lax.axis_size("lon")
    devices = nlat * nlon
    blocks = obs_count.shape[0]
    nslots = blocks * SLOTS
    big = dict(vmem_limit_bytes=60 << 20)

    rows = levels * lat_rows
    group = min(16, devices)
    each = tracers // CHAINS
    size = CAPACITY * SLOTS
    adjoint, smoothed = pl.pallas_call(
        functools.partial(exchange_kernel, tracers, levels, lat_rows, group),
        out_shape=(
            jax.ShapeDtypeStruct((tracers * rows, lanes), F32),
            jax.ShapeDtypeStruct((tracers, lat_rows, lanes), F32),
        ),
        in_specs=[VMEM] * 11,
        out_specs=(VMEM, VMEM),
        scratch_shapes=[
            pltpu.VMEM((lat_rows, lev, tracers * lanes), F32),
            pltpu.VMEM((lat_rows, 8, tracers * lanes), F32),
            pltpu.VMEM((lat_rows, lev, tracers * lanes), F32),
            pltpu.VMEM((4, lev * lat_rows, lanes), F32),
            pltpu.VMEM((2, lev * lat_rows, lanes), F32),
            pltpu.VMEM((lanes, lanes), F32),
            pltpu.VMEM((STEPS, CHAINS, 2, lev, each * lanes), BF16),
            pltpu.VMEM((STEPS, CHAINS, 2, lev, each * lanes), BF16),
            pltpu.VMEM((STEPS, CHAINS, 2, lev, lanes), BF16),
            pltpu.VMEM((STEPS, CHAINS, 2, lev, lanes), BF16),
            pltpu.SemaphoreType.DMA((STEPS, CHAINS, 2)),
            pltpu.SemaphoreType.DMA((STEPS, CHAINS, 2)),
            pltpu.SemaphoreType.DMA((STEPS, CHAINS, 2)),
            pltpu.SemaphoreType.DMA((STEPS, CHAINS, 2)),
            pltpu.VMEM((lanes, nslots), F32),
            pltpu.VMEM((blocks, SLOTS, lanes), F32),
            pltpu.VMEM((16, lanes), jnp.int32),
            pltpu.SMEM((16, lanes), jnp.int32),
            pltpu.SemaphoreType.DMA,
            pltpu.VMEM((devices, 4 * SLOTS, lanes), BF16),
            pltpu.VMEM((devices, 4 * SLOTS, lanes), BF16),
            pltpu.VMEM((lat_rows * lev, tracers * lanes), F32),
            pltpu.VMEM((group * size, lanes), F32),
            pltpu.VMEM((lat_rows * lev, group * size), BF16),
            pltpu.VMEM((group * size, tracers * lanes), BF16),
            pltpu.VMEM((lat_rows * tracers, lanes), F32),
            pltpu.VMEM((lat_rows * tracers, lanes), BF16),
            pltpu.VMEM((lat_rows * tracers, lanes), BF16),
            pltpu.VMEM((nlon, lat_rows * tracers, lanes), BF16),
            pltpu.VMEM((nlat, lat_rows * tracers, lanes), BF16),
            pltpu.VMEM((nlon * lanes, lanes), BF16),
            pltpu.VMEM((lat_rows * tracers, nlat * lat_rows * tracers), BF16),
            pltpu.SemaphoreType.DMA,
            pltpu.SemaphoreType.DMA((devices // group,)),
            pltpu.SemaphoreType.DMA((nlon,)),
            pltpu.SemaphoreType.DMA((nlon,)),
            pltpu.SemaphoreType.DMA((nlat,)),
            pltpu.SemaphoreType.DMA((nlat,)),
        ],
        compiler_params=pltpu.CompilerParams(collective_id=0, has_side_effects=True, **big),
        name="exchange",
    )(
        adjoint_in.reshape(tracers * rows, lanes),
        fractions.reshape(STEPS * 4 * rows, lanes),
        profiles.reshape(2 * rows, lanes),
        kernel,
        obs_weights,
        obs_resid,
        obs_cols.reshape(1, nslots),
        obs_owner.reshape(1, blocks),
        obs_count.reshape(1, blocks),
        lon_matrix,
        lat_matrix,
    )
    return adjoint.reshape(adjoint_in.shape), smoothed


def solution(mesh):
    placed = (
        P(None, None, "lat", "lon"),
        P(None, None, None, "lat", "lon"),
        P(None, None, "lat", "lon"),
        P(),
        P(None, ("lat", "lon")),
        P(None, ("lat", "lon")),
        P(("lat", "lon")),
        P(("lat", "lon"), None),
        P(("lat", "lon")),
        P(),
        P("lon", None),
    )
    return jax.shard_map(
        shards,
        mesh=mesh,
        in_specs=placed,
        out_specs=(P(None, None, "lat", "lon"), P(None, "lat", "lon")),
        check_vma=False,
    )
```
